32 devices in a mesh: groups: 2 (over x), dev: 16 (over z, y, core).
Axes of the slice: x: 2, y: 2, z: 4, core: 2. Of those that a mesh axis runs over, the one named last changes fastest.
Arguments:
- queries: bfloat16 [32, 512, 512], P(('groups', 'dev')), parts along dimension 0, may hold values from -120 to 120
- key_values: bfloat16 [2, 32, 512, 128], P(None, ('groups', 'dev')), parts along dimension 1, may hold values from -4 to 4
- lengths: int32 [4], P('groups'), parts along dimension 0, may hold values from 1 to 512, as said below
- out_proj: bfloat16 [4096, 2048], P('dev'), may hold values from -0.09375 to 0.09375
- residual: bfloat16 [32, 64, 2048], P(('groups', 'dev')), parts along dimension 0, may hold values from -8 to 8
- norm_gain: bfloat16 [2048], replicated, may hold values from 0.25 to 1.75
- router: bfloat16 [2048, 16], replicated, may hold values from -0.125 to 0.125
- expert_ids: int32 [32, 64, 8], P(('groups', 'dev')), parts along dimension 0, may hold values from 0 to 15, all different within a row; in each aligned block of 64 rows (0 to 63, 64 to 127, ..., all dimensions but the last counted through in order) at most 48 rows name the same one
- expert_gate_up: bfloat16 [16, 2048, 1536], P('dev'), may hold values from -0.125 to 0.125
- expert_down: bfloat16 [16, 768, 2048], P('dev'), may hold values from -0.21875 to 0.21875
Outputs:
- output: bfloat16 [32, 64, 2048], P(('groups', 'dev')), parts along dimension 0
The draws below stay inside these ranges and needn't reach their ends.
There are 2 independent parts, one for each index of `groups`. The reference program is written for one: setup_inputs(seed, part) draws one part's arguments, and reference() takes and returns one part's arrays. A program takes and returns all parts, laid end to end along the dimension named above; an argument that names none is the same for every part. Nothing has to cross between parts.
Inputs may be any that keep to these rules, and one draw needn't show every extreme that they name: `lengths`: in every draw some request has all 512 cache slots filled. Each token names 8 different experts. The tokens of one block of expert_ids name any one expert at most 48 times, and in every draw some block names some expert exactly 48 times.
All inputs are finite; a program needn't handle non-finite values.
Results may differ from the reference program's by a relative error of at most 0.011.
Values may be sent and summed in bfloat16 or wider, within the bound.
A program may use at most 128 MiB of HBM per device.

```python
import math
import jax
import jax.numpy as jnp
import numpy as np
from jax import lax

D = 2048
HEADS = 32
KV_HEADS = 4
HEAD_DIM = 128
FF = 768
TOP = 8
TOK_DEV = 64
CTX = 512
GROUP = 8
QH = 4
REQS = 2
SPAN = 512
HALF = 512
EXPERTS = 16
CAP = 48


def attention_pair(key):
    base_key = jax.random.fold_in(key, 101)
    key_query, key_pairs = jax.random.split(base_key, 2)
    block_count = GROUP * REQS
    kv_draw = jnp.clip(jax.random.normal(key_pairs, (2, block_count, HALF, HEAD_DIM), jnp.float32), -4.0, 4.0)
    query_draw = jnp.clip(2.0 * jax.random.normal(key_query, (block_count, SPAN, QH * HEAD_DIM), jnp.float32), -8.0, 8.0)
    return (query_draw, kv_draw)


def draw_queries(key, part):
    return attention_pair(key)[0].astype(jnp.bfloat16)


def draw_key_values(key, part):
    return attention_pair(key)[1].astype(jnp.bfloat16)


def draw_lengths(key, part):
    base_key = jax.random.fold_in(key, 202)
    key_len, key_full = jax.random.split(base_key)
    drawn_len = jax.random.randint(key_len, (REQS,), 1, CTX)
    filled = jax.random.randint(key_full, (), 0, REQS)
    return jnp.where(jnp.arange(REQS) == filled, CTX, drawn_len).astype(jnp.int32)


def draw_residual(key, part):
    base_key = jax.random.fold_in(key, 303)
    key_noise = jax.random.fold_in(base_key, 0)
    noise_part = jax.random.normal(key_noise, (GROUP * REQS, TOK_DEV, D), jnp.float32)
    drawn_value = 0.25 * noise_part
    return jnp.clip(drawn_value, -8.0, 8.0).astype(jnp.bfloat16)


def steps_of(stream_key, dims, cuts, least, high):
    gain = 1.0
    for position, shards_of in cuts:
        steps = jax.random.uniform(jax.random.fold_in(jax.random.fold_in(stream_key, 6), position), (shards_of,), jnp.float32, least / len(cuts), high / len(cuts))
        gain = gain * jnp.repeat(jnp.exp(steps), dims[position] // shards_of).reshape((-1,) + (1,) * (len(dims) - 1 - position))
    return gain


def routed_block(stream_key, own, number, rows, amount, top, reach, slope):
    sequence = jax.random.permutation(stream_key, amount)
    packed, usual = load_shares(amount, rows * top, reach, slope, True), load_shares(amount, rows * top, reach, slope, False)
    places = jnp.arange(amount)

    def named(sizes, offset_by):
        used = int((sizes > 0).sum())
        fixed = max(1, used // 4)
        moved = fixed + (places - fixed + offset_by * (used - fixed)) % max(1, amount - fixed)
        return jnp.zeros((amount,), jnp.int32).at[sequence[jnp.where(places < fixed, places, moved)]].set(jnp.asarray(sizes, jnp.int32))

    sizes = jnp.where(number % 4 == 0, named(packed, number // 4), named(usual, number - number // 4 - 1))
    mixed = jax.random.permutation(jax.random.fold_in(own, 3), amount)
    source_of, taker = mixed[0:amount // 2 * 2:2], mixed[1:amount // 2 * 2:2]
    room = jnp.minimum(sizes[source_of] - 1, reach - sizes[taker]) // 2
    room = jnp.where((source_of == sequence[0]) | (taker == sequence[0]) | (sizes[taker] == 0), 0, jnp.maximum(room, 0))
    moved = jax.random.randint(jax.random.fold_in(own, 4), (amount // 2,), 0, 1 << 20) % (room + 1)
    sizes = sizes.at[source_of].add(-moved).at[taker].add(moved)
    items = jnp.searchsorted(jnp.cumsum(sizes), jnp.arange(rows * top), side="right").astype(jnp.int32)
    listing = items.reshape(top, rows).T
    listing = listing[jax.random.permutation(jax.random.fold_in(own, 1), rows)]
    offset_by = jax.random.randint(jax.random.fold_in(own, 2), (rows, 1), 0, top)
    return jnp.take_along_axis(listing, (jnp.arange(top)[None, :] + offset_by) % top, axis=1)


def load_shares(number_of, total, bound, skew, full):
    weights = [(1 << 20) // math.isqrt(standing ** skew) + 1 for standing in range(1, number_of + 1)]
    largest = bound if full else min(bound, max(-(-total // number_of), total * weights[0] // sum(weights)))
    least = 1 if total - largest >= number_of - 1 else 0
    given, spare = [largest] + [least] * (number_of - 1), total - largest - least * (number_of - 1)
    while spare > 0:
        free = [i for i in range(1, number_of) if given[i] < largest] or [i for i in range(1, number_of) if given[i] < bound]
        mass, left = sum([weights[i] for i in free]), spare
        for i in free:
            addition = min(bound - given[i], max(1, left * weights[i] // mass), spare)
            given[i] = given[i] + addition
            spare = spare - addition
    return np.array(given)


def noise(rng, extent, scale, reach, cuts=(), held_as=jnp.bfloat16):
    values = scale * jax.random.normal(rng, extent, jnp.float32)
    if cuts:
        values = values * steps_of(rng, extent, cuts, -0.22, 0.18)
    return jnp.clip(values, -reach, reach).astype(held_as)


def setup_inputs(seed: int = 0, part: int = 0) -> dict:
    arg_keys = jax.random.split(jax.random.key(seed), 11)
    part_splits = jax.random.split(jax.random.fold_in(arg_keys[10], part), 11)
    queries = draw_queries(jax.random.fold_in(jax.random.fold_in(arg_keys[10], part), 71), part)
    key_values = draw_key_values(jax.random.fold_in(jax.random.fold_in(arg_keys[10], part), 71), part)
    lengths = draw_lengths(jax.random.fold_in(jax.random.fold_in(arg_keys[10], part), 71), part)
    out_proj = noise(arg_keys[3], (HEADS * HEAD_DIM, D), (HEADS * HEAD_DIM) ** -0.5, 0.09375, ((0, 16),))
    residual = draw_residual(jax.random.fold_in(jax.random.fold_in(arg_keys[10], part), 71), part)
    norm_gain = jnp.clip(1.0 + 0.15 * jax.random.normal(arg_keys[5], (D,), jnp.float32), 0.25, 1.75).astype(jnp.bfloat16)
    router = noise(arg_keys[6], (D, EXPERTS), D ** -0.5, 0.125)
    expert_ids_keys = jax.random.split(jax.random.fold_in(part_splits[7], 1), (GROUP * REQS) * TOK_DEV // TOK_DEV)
    expert_ids_turns = jax.random.permutation(jax.random.fold_in(part_splits[7], 3), (GROUP * REQS) * TOK_DEV // TOK_DEV)
    expert_ids = jax.vmap(lambda own, number: routed_block(jax.random.fold_in(part_splits[7], 2), own, number, TOK_DEV, EXPERTS, TOP, CAP, 2))(expert_ids_keys, expert_ids_turns).reshape((GROUP * REQS, TOK_DEV, TOP))
    expert_gate_up = noise(arg_keys[8], (EXPERTS, D, 2 * FF), D ** -0.5, 0.125, ((0, 16),))
    expert_down = noise(arg_keys[9], (EXPERTS, FF, D), FF ** -0.5, 0.21875, ((0, 16),))
    return dict(queries=queries, key_values=key_values, lengths=lengths, out_proj=out_proj, residual=residual, norm_gain=norm_gain, router=router, expert_ids=expert_ids, expert_gate_up=expert_gate_up, expert_down=expert_down)


EPSILON = 1e-06

def route_slots(flat_ids):
    expert_marks = (flat_ids.reshape(-1)[:, None] == jnp.arange(EXPERTS, dtype=jnp.int32)[None, :]).astype(jnp.int32)
    before = jnp.cumsum(expert_marks, axis=0) - expert_marks
    return lax.optimization_barrier(jnp.sum(before * expert_marks, axis=1)).reshape(flat_ids.shape)

def slot_rows(flat_ids, slot_index):
    positions = (flat_ids * CAP + slot_index).reshape(-1).astype(jnp.int32)
    tokens = jnp.repeat(jnp.arange(TOK_DEV, dtype=jnp.int32), TOP)
    return jnp.full((EXPERTS * CAP,), -1, jnp.int32).at[positions].set(tokens)

def expert_rows(gathered, gate_up, down_proj):
    projected = jnp.dot(gathered, gate_up, preferred_element_type=jnp.float32)
    activation = (jax.nn.silu(projected[:, :FF]) * projected[:, FF:]).astype(jnp.bfloat16)
    return jnp.dot(activation, down_proj, preferred_element_type=jnp.float32).astype(jnp.bfloat16)

def reference(queries, key_values, lengths, out_proj, residual, norm_gain, router, expert_ids, expert_gate_up, expert_down):
    block_count = GROUP * REQS
    score_scale = 1.0 / math.sqrt(HEAD_DIM)
    kv_seq = key_values.reshape(2, KV_HEADS, 2, REQS, HALF, HEAD_DIM).transpose(0, 1, 3, 2, 4, 5)
    kv_seq = kv_seq.reshape(2, KV_HEADS, REQS, 2 * HALF, HEAD_DIM)
    query_blocks = queries.reshape(block_count, SPAN, QH, HEAD_DIM)
    positions = jnp.arange(CTX + SPAN, dtype=jnp.int32)
    row_ids = jnp.arange(SPAN, dtype=jnp.int32)
    rank_ids = jnp.arange(block_count, dtype=jnp.int32) // REQS
    requests = jnp.arange(block_count, dtype=jnp.int32) % REQS

    def attend(element):
        rank_no, request, block_q = element
        key_rows = kv_seq[0, rank_no // 2, request]
        value_rows = kv_seq[1, rank_no // 2, request]
        scores = jnp.einsum('tjd,pd->jtp', block_q.astype(jnp.float32), key_rows.astype(jnp.float32)) * score_scale
        visible = (positions[None, :] < lengths[request]) | (positions[None, :] >= CTX) & (positions[None, :] - CTX <= row_ids[:, None])
        scores = jnp.where(visible[None], scores, -jnp.inf)
        row_max = lax.optimization_barrier(jnp.max(scores, axis=-1, keepdims=True))
        raised = jnp.exp(scores - row_max)
        weights = (raised / lax.optimization_barrier(jnp.sum(raised, axis=-1, keepdims=True))).astype(jnp.bfloat16)
        mixture = jnp.einsum('jtp,pd->tjd', weights.astype(jnp.float32), value_rows.astype(jnp.float32))
        return mixture.astype(jnp.bfloat16)
    head_out = lax.map(attend, (rank_ids, requests, query_blocks))
    head_out = head_out.reshape(GROUP, REQS, SPAN, QH * HEAD_DIM).transpose(1, 2, 0, 3).reshape(REQS * SPAN, HEADS * HEAD_DIM)
    attended = jnp.dot(head_out, out_proj, preferred_element_type=jnp.float32)
    attended = attended.reshape(REQS, GROUP, TOK_DEV, D).transpose(1, 0, 2, 3).reshape(block_count, TOK_DEV, D)
    stream = (residual.astype(jnp.float32) + attended).astype(jnp.bfloat16)
    values = stream.astype(jnp.float32)
    normed = (values * lax.rsqrt(lax.optimization_barrier(jnp.mean(values * values, axis=-1, keepdims=True)) + EPSILON) * norm_gain.astype(jnp.float32)).astype(jnp.bfloat16)
    logits = jnp.dot(normed.reshape(block_count * TOK_DEV, D), router, preferred_element_type=jnp.float32).reshape(block_count, TOK_DEV, EXPERTS)
    onehot = expert_ids[..., None] == jnp.arange(EXPERTS, dtype=jnp.int32)
    chosen = lax.optimization_barrier(jnp.sum(jnp.where(onehot, logits[:, :, None, :], 0.0), axis=-1))
    raised_gate = jnp.exp(chosen)
    gate_weights = raised_gate / lax.optimization_barrier(jnp.sum(raised_gate, axis=-1, keepdims=True))
    slots = jax.vmap(route_slots)(expert_ids)
    slot_table = jax.vmap(slot_rows)(expert_ids, slots)

    def visit(summed, element):
        gate_up, down_proj, expert = element
        token_pick = lax.dynamic_slice_in_dim(slot_table, (expert * CAP).astype(jnp.int32), CAP, axis=1)
        gathered = jnp.take_along_axis(normed, jnp.maximum(token_pick, 0)[:, :, None], axis=1)
        outputs = expert_rows(gathered.reshape(block_count * CAP, D), gate_up, down_proj).reshape(block_count, CAP, D)
        is_chosen = expert_ids == expert
        weight = lax.optimization_barrier(jnp.sum(jnp.where(is_chosen, gate_weights, 0.0), axis=2))
        slot_pick = lax.optimization_barrier(jnp.sum(jnp.where(is_chosen, slots, 0), axis=2)).astype(jnp.int32)
        picked = jnp.take_along_axis(outputs, slot_pick[:, :, None], axis=1)
        return (summed + weight[:, :, None] * picked.astype(jnp.float32), None)
    summed, _ = lax.scan(visit, jnp.zeros((block_count, TOK_DEV, D), jnp.float32), (expert_gate_up, expert_down, jnp.arange(EXPERTS, dtype=jnp.int32)))
    return (values + summed).astype(jnp.bfloat16)
```

```python
import functools
import math

import jax
import jax.numpy as jnp
from jax import lax
from jax.experimental import pallas as pl
from jax.experimental.pallas import tpu as pltpu
from jax.sharding import PartitionSpec as P

HEAD_DIM = 128
FF = 768
TOK_DEV = 64
GROUP = 8
EPSILON = 1e-06
MESH = pl.DeviceIdType.MESH
CHUNKS = 4
AG_KINDS = (0, 1, 0, 0)
RS_KINDS = (0, 1, 0, 0)
AG_FIRST = 1.0
AG_CHUNK = 1.0
AG_HOP = 1.0
FFN_START = 4.0
FFN_CHUNK = 1.0
FFN_SPAN = 0.9
RS_LAG = 0.5
RS_HOP = 1.0


def bit_count(number):
    return number.bit_length() - 1


def flipped(index, bits):
    for bit in bits:
        index = index + (1 - 2 * ((index // (1 << bit)) % 2)) * (1 << bit)
    return index


def subset(bits, number):
    return [bit for place, bit in enumerate(bits) if number >> place & 1]


def greet(me, bits):
    barrier = pltpu.get_barrier_semaphore()
    for bit in bits:
        pl.semaphore_signal(
            barrier, inc=1, device_id={"dev": flipped(me, [bit])}, device_id_type=MESH
        )
    pl.semaphore_wait(barrier, len(bits))


def scatter_steps(me, unit, part_no, order, cols, x_ref, recv, stage, send_sem, recv_sem, block_of):
    k = len(order)
    total = (1 << k) - 1
    first = [total - ((1 << (k - s)) - 1) for s in range(k)]

    def arrived(step, number):
        return pltpu.make_async_remote_copy(
            src_ref=recv.at[first[step] + number, :, cols],
            dst_ref=recv.at[first[step] + number, :, cols],
            send_sem=send_sem.at[part_no, first[step] + number],
            recv_sem=recv_sem.at[part_no, first[step] + number],
            device_id={"dev": flipped(me, [unit + order[step]])},
            device_id_type=MESH,
        )

    copies = []

    def send(step, only=None):
        for number in reversed(range(1 << (k - 1 - step))) if only is None else [only]:
            slot = first[step] + number
            flips = [order[step]] + subset(order[step + 1 :], number)
            block = block_of(flips)
            if step == 0:
                source = x_ref.at[block, :, cols]
            else:
                value = x_ref[block, :, cols].astype(jnp.float32)
                for earlier in range(step):
                    place = (1 << (step - earlier - 1)) + (number << (step - earlier))
                    arrived(earlier, place).wait_recv()
                    value = value + recv[first[earlier] + place, :, cols].astype(jnp.float32)
                spot = slot - first[1]
                stage[spot, :, cols] = value.astype(stage.dtype)
                source = stage.at[spot, :, cols]
            copy = pltpu.make_async_remote_copy(
                src_ref=source,
                dst_ref=recv.at[slot, :, cols],
                send_sem=send_sem.at[part_no, slot],
                recv_sem=recv_sem.at[part_no, slot],
                device_id={"dev": flipped(me, [unit + order[step]])},
                device_id_type=MESH,
            )
            copy.start()
            copies.append(copy)

    def finish(o_ref):
        value = x_ref[block_of([]), :, cols].astype(jnp.float32)
        for earlier in range(k):
            arrived(earlier, 0).wait_recv()
            value = value + recv[first[earlier], :, cols].astype(jnp.float32)
        o_ref[:, cols] = value
        for copy in copies:
            copy.wait_send()

    return send, finish


def scatter_kernel(unit, parts, bits, x_ref, o_ref, recv, stage, send_sem, recv_sem):
    me = lax.axis_index("dev")
    greet(me, [unit + bit for bit in bits])
    rank = me // (1 << unit)
    runs = [
        scatter_steps(
            me, unit, number, order, cols, x_ref, recv, stage, send_sem, recv_sem,
            lambda flips: flipped(rank, flips),
        )
        for number, (order, cols) in enumerate(parts)
    ]
    for step in range(len(bits)):
        for send, _ in runs:
            send(step)
    for _, finish in runs:
        finish(o_ref)


def attend_block(block, length, q_ref, halves, rows):
    heads = q_ref.shape[1] // HEAD_DIM
    picked = pl.ds(pl.multiple_of(block * rows, rows), rows)
    query = jnp.concatenate(
        [q_ref[picked, head * HEAD_DIM : (head + 1) * HEAD_DIM] for head in range(heads)], axis=0
    )
    scale = 1.0 / math.sqrt(HEAD_DIM)
    contract = (((1,), (1,)), ((), ()))
    old = lax.dot_general(query, halves[0, 0], contract, preferred_element_type=jnp.float32) * scale
    new = lax.dot_general(query, halves[1, 0], contract, preferred_element_type=jnp.float32) * scale
    column = lax.broadcasted_iota(jnp.int32, (1, old.shape[1]), 1)
    old = jnp.where(column < length, old, -1e30)
    column = lax.broadcasted_iota(jnp.int32, (rows, new.shape[1]), 1)
    token = lax.broadcasted_iota(jnp.int32, (rows, new.shape[1]), 0) + block * rows
    bias = jnp.where(column <= token, 0.0, -1e30)
    new = new + jnp.concatenate([bias] * heads, axis=0)
    top = jnp.maximum(jnp.max(old, axis=1, keepdims=True), jnp.max(new, axis=1, keepdims=True))
    old = jnp.exp(old - top)
    new = jnp.exp(new - top)
    total = jnp.sum(old, axis=1, keepdims=True) + jnp.sum(new, axis=1, keepdims=True)
    mixed = jnp.dot(old.astype(jnp.bfloat16), halves[0, 1], preferred_element_type=jnp.float32)
    mixed += jnp.dot(new.astype(jnp.bfloat16), halves[1, 1], preferred_element_type=jnp.float32)
    mixed = (mixed / total).astype(jnp.bfloat16)
    return jnp.concatenate(
        [mixed[head * rows : (head + 1) * rows] for head in range(heads)], axis=1
    )


def attention_kernel(
    unit, parts, bits,
    lengths_ref, q_ref, kv_ref, proj_ref, o_ref,
    halves, proj, heads, x, recv, stage,
    send_sem, recv_sem, kv_sem, proj_send, proj_recv, own_sem,
):
    me = lax.axis_index("dev")
    low = list(range(unit))
    mates = [flipped(me, subset(low, number)) for number in range(1, 1 << unit)]
    ranks = [flipped(me, [unit + bit]) for bit in bits]
    barrier = pltpu.get_barrier_semaphore()
    for other in mates + ranks:
        pl.semaphore_signal(barrier, inc=1, device_id={"dev": other}, device_id_type=MESH)
    request = me % (1 << unit)
    rank = me // (1 << unit)
    parity = rank % 2
    depth = proj_ref.shape[0]
    own_rows = pl.ds(pl.multiple_of(request * depth, depth), depth)
    own_half = pltpu.make_async_copy(kv_ref, halves.at[parity], own_sem.at[0])
    own_proj = pltpu.make_async_copy(proj_ref, proj.at[own_rows], own_sem.at[1])
    own_half.start()
    own_proj.start()
    pl.semaphore_wait(barrier, len(mates) + len(ranks))
    kv_copy = pltpu.make_async_remote_copy(
        src_ref=kv_ref,
        dst_ref=halves.at[parity],
        send_sem=kv_sem.at[0],
        recv_sem=kv_sem.at[1],
        device_id={"dev": ranks[0]},
        device_id_type=MESH,
    )
    kv_copy.start()
    proj_copies = []
    for place, other in enumerate(mates):
        copy = pltpu.make_async_remote_copy(
            src_ref=proj_ref,
            dst_ref=proj.at[own_rows],
            send_sem=proj_send.at[place],
            recv_sem=proj_recv.at[place],
            device_id={"dev": other},
            device_id_type=MESH,
        )
        copy.start()
        proj_copies.append(copy)
    own_half.wait()
    kv_copy.wait()

    blocks, rows, width = x.shape
    far = 1 << (len(bits) - 1)
    masks = sorted(range(blocks), key=lambda m: (-bin(m).count("1"), -(m & far), m))
    place_of = {mask: place for place, mask in enumerate(masks)}
    length = lengths_ref[request]
    runs = [
        scatter_steps(
            me, unit, number, order, cols, x, recv, stage, send_sem, recv_sem,
            lambda flips: place_of[sum(1 << bit for bit in flips)],
        )
        for number, (order, cols) in enumerate(parts)
    ]
    half = blocks // 2
    strip = math.gcd(width, 512)
    for group in range(2):
        for spot in range(half):
            mask = masks[group * half + spot]
            block = flipped(rank, subset(bits, mask))
            heads[spot * rows : (spot + 1) * rows, :] = attend_block(
                block, length, q_ref, halves, rows
            )
        if group == 0:
            own_proj.wait()
            for copy in proj_copies:
                copy.wait()
        for start in range(0, width, strip):
            product = jnp.dot(
                heads[...], proj[:, start : start + strip], preferred_element_type=jnp.float32
            ).astype(x.dtype)
            for spot in range(half):
                x[group * half + spot, :, start : start + strip] = product[
                    spot * rows : (spot + 1) * rows
                ]
        for spot in range(half):
            mask = masks[group * half + spot]
            for (send, _), (order, _) in zip(runs, parts):
                if mask >> order[0] & 1:
                    number = sum((mask >> bit & 1) << at for at, bit in enumerate(order[1:]))
                    send(0, number)
    for step in range(1, len(bits)):
        for send, _ in runs:
            send(step)
    for _, finish in runs:
        finish(o_ref)


def attention(lengths, queries, key_values, out_proj, unit, orders, collective_id):
    width = out_proj.shape[1]
    tokens, columns = queries.shape
    bits = sorted(orders[0])
    blocks = 1 << len(bits)
    rows = tokens // blocks
    cut = width * 3 // 4 // 128 * 128
    parts = [(orders[0], pl.ds(0, cut)), (orders[1], pl.ds(cut, width - cut))]
    mates = max((1 << unit) - 1, 1)
    kind = queries.dtype
    whole = pl.BlockSpec(memory_space=pltpu.VMEM)
    return pl.pallas_call(
        functools.partial(attention_kernel, unit, parts, bits),
        out_shape=jax.ShapeDtypeStruct((rows, width), jnp.float32),
        in_specs=[pl.BlockSpec(memory_space=pltpu.SMEM), whole, whole, whole],
        out_specs=whole,
        scratch_shapes=[
            pltpu.VMEM((2,) + key_values.shape, kind),
            pltpu.VMEM((out_proj.shape[0] << unit, width), kind),
            pltpu.VMEM((tokens // 2, columns), kind),
            pltpu.VMEM((blocks, rows, width), kind),
            pltpu.VMEM((blocks - 1, rows, width), kind),
            pltpu.VMEM((max(blocks // 2 - 1, 1), rows, width), kind),
            pltpu.SemaphoreType.DMA((2, blocks - 1)),
            pltpu.SemaphoreType.DMA((2, blocks - 1)),
            pltpu.SemaphoreType.DMA((2,)),
            pltpu.SemaphoreType.DMA((mates,)),
            pltpu.SemaphoreType.DMA((mates,)),
            pltpu.SemaphoreType.DMA((2,)),
        ],
        compiler_params=pltpu.CompilerParams(collective_id=collective_id, has_side_effects=True),
    )(lengths, queries, key_values, out_proj)


def reduce_scatter(x, unit, orders, collective_id):
    blocks, rows, width = x.shape
    bits = sorted(orders[0])
    cut = width * 3 // 4 // 128 * 128
    parts = [(orders[0], pl.ds(0, cut)), (orders[1], pl.ds(cut, width - cut))]
    return pl.pallas_call(
        functools.partial(scatter_kernel, unit, parts, bits),
        out_shape=jax.ShapeDtypeStruct((rows, width), jnp.float32),
        in_specs=[pl.BlockSpec(memory_space=pltpu.VMEM)],
        out_specs=pl.BlockSpec(memory_space=pltpu.VMEM),
        scratch_shapes=[
            pltpu.VMEM((blocks - 1, rows, width), x.dtype),
            pltpu.VMEM((max(blocks // 2 - 1, 1), rows, width), x.dtype),
            pltpu.SemaphoreType.DMA((2, blocks - 1)),
            pltpu.SemaphoreType.DMA((2, blocks - 1)),
        ],
        compiler_params=pltpu.CompilerParams(collective_id=collective_id, has_side_effects=True),
    )(x)


def gather_kernel(parts, bits, x_ref, g_ref, ox_ref, og_ref, send_sem, recv_sem, own_sem):
    me = lax.axis_index("dev")
    greet(me, bits)
    k = len(bits)
    pairs = [(x_ref, ox_ref), (g_ref, og_ref)]
    local = []
    for number, (source, target) in enumerate(pairs):
        copy = pltpu.make_async_copy(source, target.at[me], own_sem.at[number])
        copy.start()
        local.append(copy)
    sent = []

    def forward(part_no, held, step):
        which, order, cols = parts[part_no]
        source, target = pairs[which]
        block = flipped(me, subset(order, held))
        slot = (1 << step) - 1 + held
        copy = pltpu.make_async_remote_copy(
            src_ref=source.at[:, cols] if held == 0 else target.at[block, :, cols],
            dst_ref=target.at[block, :, cols],
            send_sem=send_sem.at[part_no, slot],
            recv_sem=recv_sem.at[part_no, slot],
            device_id={"dev": flipped(me, [order[step]])},
            device_id_type=MESH,
        )
        copy.start()
        sent.append(copy)

    def arrive(part_no, held, step):
        which, order, cols = parts[part_no]
        target = pairs[which][1]
        block = flipped(me, subset(order, held) + [order[step]])
        slot = (1 << step) - 1 + held
        pltpu.make_async_remote_copy(
            src_ref=target.at[block, :, cols],
            dst_ref=target.at[block, :, cols],
            send_sem=send_sem.at[part_no, slot],
            recv_sem=recv_sem.at[part_no, slot],
            device_id={"dev": flipped(me, [order[step]])},
            device_id_type=MESH,
        ).wait_recv()

    for step in range(k):
        for part_no in range(len(parts)):
            forward(part_no, 0, step)
    for step in range(k):
        for held in range(1 << step):
            for part_no in range(len(parts)):
                arrive(part_no, held, step)
                for later in range(step + 1, k):
                    forward(part_no, held + (1 << step), later)
    for copy in local:
        copy.wait()
    for copy in sent:
        copy.wait_send()


def all_gather(x, gates, orders, collective_id):
    rows, width = x.shape
    bits = sorted(orders[0])
    count = 1 << len(bits)
    cut = width * 3 // 4 // 128 * 128
    parts = [
        (1, orders[0], pl.ds(0, gates.shape[1])),
        (0, orders[0], pl.ds(0, cut)),
        (0, orders[1], pl.ds(cut, width - cut)),
    ]
    return pl.pallas_call(
        functools.partial(gather_kernel, parts, bits),
        out_shape=[
            jax.ShapeDtypeStruct((count, rows, width), x.dtype),
            jax.ShapeDtypeStruct((count,) + gates.shape, gates.dtype),
        ],
        in_specs=[pl.BlockSpec(memory_space=pltpu.VMEM)] * 2,
        out_specs=[pl.BlockSpec(memory_space=pltpu.VMEM)] * 2,
        scratch_shapes=[
            pltpu.SemaphoreType.DMA((3, count - 1)),
            pltpu.SemaphoreType.DMA((3, count - 1)),
            pltpu.SemaphoreType.DMA((2,)),
        ],
        compiler_params=pltpu.CompilerParams(collective_id=collective_id, has_side_effects=True),
    )(x, gates)


def ag_time(k, stage):
    return AG_CHUNK * k + AG_HOP * stage if stage else AG_FIRST * k


def ffn_time(k, part):
    return FFN_START + FFN_CHUNK * k + FFN_SPAN * part + 0.001


def rs_time(k, stage):
    return FFN_START + FFN_CHUNK * k + FFN_SPAN + RS_LAG + RS_HOP * stage


def moe_fits(devices, rows, width, hidden):
    if devices < 8 or rows % (16 * CHUNKS):
        return False
    weights = 3 * width * hidden
    tokens = devices * rows * width
    return 2 * (weights + 4 * tokens) < 48 * 2**20


def moe_kernel(
    line, ag_kinds, rs_kinds,
    att_ref, res_ref, gain_ref, router_ref, ids_ref, gu_hbm, dn_hbm, o_ref,
    gath, gu, dn, act, made, mrecv, part, yrecv, half, zrecv, held, ready,
    w_sem, ag_send, ag_recv, m_send, m_recv, y_send, y_recv, z_send, z_recv,
):
    me = lax.axis_index("dev")
    z, y, c = me // 4, (me // 2) % 2, me % 2
    chunks, total, padded = gath.shape
    rows, width = o_ref.shape
    R = rows // chunks
    hidden = dn.shape[0]
    experts = router_ref.shape[0]
    dest = [me + 4, me - 4, me + 2 - 4 * y, me + 1 - 2 * c]
    allowed = [z + 1 < line, z > 0, None, None]
    RIGHT, LEFT, YMATE, MATE = range(4)

    def guarded(cond, body):
        if cond is None:
            body()
        else:
            pl.when(cond)(body)

    def both(*conds):
        conds = [cond for cond in conds if cond is not None]
        if not conds:
            return None
        return functools.reduce(jnp.logical_and, conds)

    copies = [
        pltpu.make_async_copy(gu_hbm.at[0], gu, w_sem.at[0]),
        pltpu.make_async_copy(dn_hbm.at[0], dn, w_sem.at[1]),
    ]
    for copy in copies:
        copy.start()
    barrier = pltpu.get_barrier_semaphore()
    for way in range(4):
        guarded(
            allowed[way],
            lambda way=way: pl.semaphore_signal(
                barrier, inc=1, device_id={"dev": dest[way]}, device_id_type=MESH
            ),
        )

    stream = (res_ref[...].astype(jnp.float32) + att_ref[...]).astype(jnp.bfloat16)
    values = stream.astype(jnp.float32)
    held[...] = values
    scale = lax.rsqrt(jnp.mean(values * values, axis=-1, keepdims=True) + EPSILON)
    normed = (values * scale * gain_ref[...].astype(jnp.float32).reshape(1, width)).astype(jnp.bfloat16)
    logits = lax.dot_general(
        router_ref[...], normed, (((1,), (1,)), ((), ())), preferred_element_type=jnp.float32
    )
    number = lax.broadcasted_iota(jnp.int32, (experts, rows), 0)
    named = ids_ref[0:1, :] == number
    for place in range(1, ids_ref.shape[0]):
        named = jnp.logical_or(named, ids_ref[place : place + 1, :] == number)
    raised = jnp.where(named, jnp.exp(logits), 0.0)
    gates = raised / jnp.sum(raised, axis=0, keepdims=True)
    high = gates.astype(jnp.bfloat16).astype(jnp.float32)
    low = gates - high
    spare = jnp.zeros((padded - width - 2 * experts, rows), jnp.float32)
    extra = jnp.concatenate([high, low, spare], axis=0).T.astype(jnp.bfloat16)

    def spot(core, column, place):
        return pl.multiple_of(((core * 2 + column) * line + place) * R, R)

    mine = pl.ds(spot(c, y, z), R)
    for k in range(chunks):
        gath[k, mine, 0:width] = normed[k * R : (k + 1) * R]
        gath[k, mine, width:padded] = extra[k * R : (k + 1) * R]

    pl.semaphore_wait(
        barrier, 2 + (z > 0).astype(jnp.int32) + (z + 1 < line).astype(jnp.int32)
    )

    span = 2 * line - 1
    started = []

    def label(side, offset):
        return side * span + offset + line - 1

    def exists(offset):
        if offset == 0:
            return None
        return z + offset >= 0 if offset < 0 else z + offset < line

    def slab(k, side, offset):
        column = y if side == 0 else 1 - y
        return gath.at[k, pl.ds(spot(c, column, z + offset), R), :]

    def ag_copy(k, side, offset, way):
        if way == RIGHT:
            landing = label(side, offset - 1)
        elif way == LEFT:
            landing = label(side, offset + 1)
        elif way == YMATE:
            landing = label(1 - side, offset)
        else:
            landing = 2 * span + label(side, offset)
        where = slab(k, side, offset)
        return pltpu.make_async_remote_copy(
            src_ref=where, dst_ref=where,
            send_sem=ag_send.at[k, label(side, offset), way],
            recv_sem=ag_recv.at[k, landing],
            device_id={"dev": dest[way]}, device_id_type=MESH,
        )

    def ag_ways(k, side, offset):
        kind = ag_kinds[k]
        ways = []
        if kind == 0:
            if side == 0:
                if offset <= 0 and offset > 1 - line:
                    ways.append(RIGHT)
                if offset >= 0 and offset < line - 1:
                    ways.append(LEFT)
                ways.append(YMATE)
        else:
            if side == 0 and offset == 0:
                ways.append(YMATE)
            if offset <= 0 and offset > 1 - line:
                ways.append(RIGHT)
            if offset >= 0 and offset < line - 1:
                ways.append(LEFT)
        ways.append(MATE)
        return ways

    def ag_step(k, side, offset):
        def body():
            if side or offset:
                arrived = slab(k, side, offset)
                pltpu.make_async_remote_copy(
                    src_ref=arrived, dst_ref=arrived,
                    send_sem=ag_send.at[k, label(side, offset), MATE],
                    recv_sem=ag_recv.at[k, label(side, offset)],
                    device_id={"dev": dest[MATE]}, device_id_type=MESH,
                ).wait_recv()
            for way in ag_ways(k, side, offset):
                copy = ag_copy(k, side, offset, way)
                guarded(allowed[way], copy.start)

        guarded(exists(offset), body)
        for way in ag_ways(k, side, offset):
            started.append(
                (
                    lambda way=way: both(exists(offset), allowed[way]),
                    lambda way=way: ag_copy(k, side, offset, way),
                )
            )

    def ag_stage(k, stage):
        if stage == 0:
            ag_step(k, 0, 0)
            return
        if stage < line:
            ag_step(k, 0, -stage)
            ag_step(k, 0, stage)
        if stage == 1:
            ag_step(k, 1, 0)
        else:
            ag_step(k, 1, 1 - stage)
            ag_step(k, 1, stage - 1)

    def mate_wait(k):
        for side in range(2):
            for offset in range(1 - line, line):
                column = y if side == 0 else 1 - y

                def body(side=side, offset=offset, column=column):
                    where = gath.at[k, pl.ds(spot(1 - c, column, z + offset), R), :]
                    pltpu.make_async_remote_copy(
                        src_ref=where, dst_ref=where,
                        send_sem=ag_send.at[k, label(side, offset), MATE],
                        recv_sem=ag_recv.at[k, 2 * span + label(side, offset)],
                        device_id={"dev": dest[MATE]}, device_id_type=MESH,
                    ).wait_recv()

                guarded(exists(offset), body)

    core_rows = total // 2
    strip = math.gcd(hidden, 256)

    wide = math.gcd(width, 512)

    def rise(k, start):
        if start == 0:
            if k == 0:
                for copy in copies:
                    copy.wait()
            mate_wait(k)
        x = gath[k, :, 0:width]
        if True:
            gate = jnp.dot(x, gu[:, start : start + strip], preferred_element_type=jnp.float32)
            up = jnp.dot(
                x, gu[:, hidden + start : hidden + start + strip],
                preferred_element_type=jnp.float32,
            )
            act[:, start : start + strip] = (gate / (1.0 + jnp.exp(-gate)) * up).astype(act.dtype)

    def fall(k, start):
        tail = gath[k, :, width:padded].astype(jnp.float32)
        lanes = lax.broadcasted_iota(jnp.int32, tail.shape, 1)
        chosen = jnp.logical_or(lanes == me, lanes == me + experts)
        weight = jnp.sum(jnp.where(chosen, tail, 0.0), axis=1, keepdims=True)
        if True:
            produced = jnp.dot(
                act[...], dn[:, start : start + wide], preferred_element_type=jnp.float32
            )
            made[k, :, start : start + wide] = (weight * produced).astype(made.dtype)
        if start + wide == width:
            mate_copy(k).start()
            started.append((lambda: None, lambda: mate_copy(k)))

    def mate_copy(k):
        theirs = pl.ds(pl.multiple_of((1 - c) * core_rows, core_rows), core_rows)
        return pltpu.make_async_remote_copy(
            src_ref=made.at[k, theirs, :], dst_ref=mrecv.at[k],
            send_sem=m_send.at[k], recv_sem=m_recv.at[k],
            device_id={"dev": dest[MATE]}, device_id_type=MESH,
        )

    def y_copy(k):
        if rs_kinds[k] == 0:
            source, target = part.at[k, 1 - y], yrecv.at[k]
        else:
            source, target = ready.at[k], yrecv.at[k, 0]
        return pltpu.make_async_remote_copy(
            src_ref=source, dst_ref=target,
            send_sem=y_send.at[k], recv_sem=y_recv.at[k],
            device_id={"dev": dest[YMATE]}, device_id_type=MESH,
        )

    def z_copy(k, target, way):
        if rs_kinds[k] == 0:
            source, landing = half.at[k, target], zrecv.at[k, way, target, 0]
        else:
            source, landing = part.at[k, :, target], zrecv.at[k, way, target]
        return pltpu.make_async_remote_copy(
            src_ref=source, dst_ref=landing,
            send_sem=z_send.at[k, way, target], recv_sem=z_recv.at[k, way, target],
            device_id={"dev": dest[way]}, device_id_type=MESH,
        )

    def merge(k):
        mate_copy(k).wait_recv()
        for column in range(2):
            for place in range(line):
                at = column * line + place
                ours = pl.ds(pl.multiple_of(c * core_rows + at * R, R), R)
                part[k, column, place] = (
                    made[k, ours, :].astype(jnp.float32)
                    + mrecv[k, at * R : (at + 1) * R, :].astype(jnp.float32)
                ).astype(part.dtype)
        if rs_kinds[k] == 0:
            y_copy(k).start()
            started.append((lambda: None, lambda: y_copy(k)))

    def y_merge(k):
        y_copy(k).wait_recv()
        for place in range(line):
            half[k, place] = (
                part[k, y, place].astype(jnp.float32) + yrecv[k, place].astype(jnp.float32)
            ).astype(half.dtype)

    def z_hop(k, hop):
        for way in (RIGHT, LEFT):
            here = hop if way == RIGHT else line - 1 - hop
            if way == RIGHT:
                targets = range(line - 1, here, -1)
            else:
                targets = range(0, here)

            def body(way=way, here=here, targets=targets):
                for target in targets:
                    if hop:
                        z_copy(k, target, way).wait_recv()
                        if rs_kinds[k] == 0:
                            half[k, target] = (
                                half[k, target].astype(jnp.float32)
                                + zrecv[k, way, target, 0].astype(jnp.float32)
                            ).astype(half.dtype)
                        else:
                            for column in range(2):
                                part[k, column, target] = (
                                    part[k, column, target].astype(jnp.float32)
                                    + zrecv[k, way, target, column].astype(jnp.float32)
                                ).astype(part.dtype)
                    z_copy(k, target, way).start()

            for target in targets:
                started.append(
                    (
                        lambda here=here: z == here,
                        lambda target=target, way=way: z_copy(k, target, way),
                    )
                )
            pl.when(z == here)(body)

    def gather_z(k, column):
        where = pl.ds(k * R, R)

        def take(way):
            side = 0 if rs_kinds[k] == 0 else column
            held[where, :] = held[where, :] + zrecv[k, way, z, side].astype(jnp.float32)

        pl.when(z > 0)(lambda: take(RIGHT))
        pl.when(z + 1 < line)(lambda: take(LEFT))

    def wait_z(k):
        pl.when(z > 0)(lambda: z_copy(k, z, RIGHT).wait_recv())
        pl.when(z + 1 < line)(lambda: z_copy(k, z, LEFT).wait_recv())

    def cross(k):
        wait_z(k)
        other = part[k, 1 - y, z].astype(jnp.float32)
        from_left = zrecv[k, RIGHT, z, 1 - y].astype(jnp.float32)
        from_right = zrecv[k, LEFT, z, 1 - y].astype(jnp.float32)
        other = other + jnp.where(z > 0, from_left, 0.0)
        other = other + jnp.where(z + 1 < line, from_right, 0.0)
        ready[k] = other.astype(ready.dtype)
        y_copy(k).start()
        started.append((lambda: None, lambda: y_copy(k)))

    def finish(k):
        where = pl.ds(k * R, R)
        if rs_kinds[k] == 0:
            wait_z(k)
            held[where, :] = held[where, :] + half[k, z].astype(jnp.float32)
            gather_z(k, 0)
            o_ref[where, :] = held[where, :].astype(o_ref.dtype)
        else:
            held[where, :] = held[where, :] + part[k, y, z].astype(jnp.float32)
            gather_z(k, y)
            y_copy(k).wait_recv()
            o_ref[where, :] = (
                held[where, :] + yrecv[k, 0].astype(jnp.float32)
            ).astype(o_ref.dtype)

    def rs_stages(k):
        hops = [functools.partial(z_hop, k, hop) for hop in range(line - 1)]
        if rs_kinds[k] == 0:
            middle = [lambda: y_merge(k)] + hops
        else:
            middle = hops + [lambda: cross(k)]
        return [lambda: merge(k)] + middle + [lambda: finish(k)]

    pieces = [functools.partial(rise, start=start) for start in range(0, hidden, strip)]
    pieces += [functools.partial(fall, start=start) for start in range(0, width, wide)]
    agenda = []
    for k in range(chunks):
        for stage in range(line + 1):
            agenda.append((ag_time(k, stage), lambda k=k, stage=stage: ag_stage(k, stage)))
        for number, piece in enumerate(pieces):
            agenda.append((ffn_time(k, number / len(pieces)), lambda k=k, piece=piece: piece(k)))
        for number, step in enumerate(rs_stages(k)):
            agenda.append((rs_time(k, number), step))
    for _, step in sorted(agenda, key=lambda entry: entry[0]):
        step()
    for cond, copy in started:
        guarded(cond(), lambda copy=copy: copy().wait_send())


def moe(attended, residual, gain, router, ids, gate_up, down, collective_id):
    devices = lax.axis_size("dev")
    rows, width = residual.shape
    hidden = down.shape[1]
    experts = router.shape[0]
    line = devices // 4
    padded = width + -(-2 * experts // 128) * 128
    R = rows // CHUNKS
    kind = residual.dtype
    span = 2 * line - 1
    vmem = pl.BlockSpec(memory_space=pltpu.VMEM)
    hbm = pl.BlockSpec(memory_space=pl.ANY)
    dma = pltpu.SemaphoreType.DMA
    total = devices * R
    return pl.pallas_call(
        functools.partial(moe_kernel, line, AG_KINDS, RS_KINDS),
        out_shape=jax.ShapeDtypeStruct((rows, width), kind),
        in_specs=[vmem] * 5 + [hbm] * 2,
        out_specs=vmem,
        scratch_shapes=[
            pltpu.VMEM((CHUNKS, total, padded), kind),
            pltpu.VMEM(gate_up.shape[1:], kind),
            pltpu.VMEM(down.shape[1:], kind),
            pltpu.VMEM((total, hidden), kind),
            pltpu.VMEM((CHUNKS, total, width), kind),
            pltpu.VMEM((CHUNKS, total // 2, width), kind),
            pltpu.VMEM((CHUNKS, 2, line, R, width), kind),
            pltpu.VMEM((CHUNKS, line, R, width), kind),
            pltpu.VMEM((CHUNKS, line, R, width), kind),
            pltpu.VMEM((CHUNKS, 2, line, 2, R, width), kind),
            pltpu.VMEM((rows, width), jnp.float32),
            pltpu.VMEM((CHUNKS, R, width), kind),
            dma((2,)),
            dma((CHUNKS, 2 * span, 4)),
            dma((CHUNKS, 4 * span)),
            dma((CHUNKS,)),
            dma((CHUNKS,)),
            dma((CHUNKS,)),
            dma((CHUNKS,)),
            dma((CHUNKS, 2, line)),
            dma((CHUNKS, 2, line)),
        ],
        compiler_params=pltpu.CompilerParams(collective_id=collective_id, has_side_effects=True),
    )(attended, residual, gain, router, ids, gate_up, down)


def swapped(order, one, two):
    order = list(order)
    order[one], order[two] = order[two], order[one]
    return order


def per_device(
    queries,
    key_values,
    lengths,
    out_proj,
    residual,
    norm_gain,
    router,
    expert_ids,
    expert_gate_up,
    expert_down,
):
    devices = lax.axis_size("dev")
    my_index = lax.axis_index("dev")
    width = residual.shape[-1]
    requests_n = devices // GROUP
    low_bits = bit_count(requests_n)
    near = list(range(bit_count(GROUP)))
    attended = attention(
        lengths, queries[0], key_values[:, 0], out_proj, low_bits, [near, swapped(near, 0, 1)], 1
    )
    if moe_fits(devices, TOK_DEV, width, FF):
        return moe(
            attended, residual[0], norm_gain, router.T, expert_ids[0].T,
            expert_gate_up, expert_down, 2,
        )[None]
    stream = (residual[0].astype(jnp.float32) + attended).astype(jnp.bfloat16)
    values = stream.astype(jnp.float32)
    normed = (
        values
        * lax.rsqrt(jnp.mean(values * values, axis=-1, keepdims=True) + EPSILON)
        * norm_gain.astype(jnp.float32)
    ).astype(jnp.bfloat16)
    logits = jnp.dot(normed, router, preferred_element_type=jnp.float32)
    experts_n = router.shape[1]
    token_ids = expert_ids[0]
    named = jnp.any(token_ids[..., None] == jnp.arange(experts_n, dtype=jnp.int32), axis=1)
    raised_gate = jnp.where(named, jnp.exp(logits), 0.0)
    gates = raised_gate / jnp.sum(raised_gate, axis=-1, keepdims=True)
    lanes = -(-TOK_DEV // 128) * 128
    gates = jnp.pad(gates.T, ((0, 0), (0, lanes - TOK_DEV)))
    every = list(range(bit_count(devices)))
    far = every[::-1]
    count = len(far)
    rows_all, gates_all = all_gather(normed, gates, [far, swapped(far, count - 3, count - 2)], 2)
    my_gates = lax.dynamic_index_in_dim(gates_all, my_index, 1, keepdims=False)[:, :TOK_DEV]
    flat_rows = rows_all.reshape(devices * TOK_DEV, width)
    projected = jnp.dot(flat_rows, expert_gate_up[0], preferred_element_type=jnp.float32)
    activation = (jax.nn.silu(projected[:, :FF]) * projected[:, FF:]).astype(jnp.bfloat16)
    produced = jnp.dot(activation, expert_down[0], preferred_element_type=jnp.float32)
    weighted = (my_gates.reshape(-1, 1) * produced).astype(jnp.bfloat16)
    weighted = weighted.reshape(devices, TOK_DEV, width)
    combined = reduce_scatter(weighted, 0, [every, swapped(every, 1, 2)], 3)
    return (values + combined).astype(jnp.bfloat16)[None]


def solution(mesh):
    return jax.shard_map(
        per_device,
        mesh=mesh,
        in_specs=(
            P(("groups", "dev"), None, None),
            P(None, ("groups", "dev"), None, None),
            P("groups"),
            P("dev", None),
            P(("groups", "dev"), None, None),
            P(),
            P(),
            P(("groups", "dev"), None, None),
            P("dev", None, None),
            P("dev", None, None),
        ),
        out_specs=P(("groups", "dev"), None, None),
        check_vma=False,
    )
```

```python
import functools
import math

import jax
import jax.numpy as jnp
from jax import lax
from jax.experimental import pallas as pl
from jax.experimental.pallas import tpu as pltpu
from jax.sharding import PartitionSpec as P

HEAD_DIM = 128
FF = 768
TOK_DEV = 64
GROUP = 8
EPSILON = 1e-06
MESH = pl.DeviceIdType.MESH
CHUNKS = 4
AG_KINDS = (0, 1, 0, 1)
ORDER = (
    0, 1, 0, 1, 0, 2, 0, 0, 1, 2, 1, 0, 3, 0, 0, 0, 0, 0, 2, 1, 0, 1, 3, 2,
    1, 0, 1, 1, 1, 1, 2, 1, 2, 3, 2, 2, 1, 2, 3, 2, 2, 0, 0, 3, 2, 3, 3, 3,
    3, 2, 3, 3, 3, 1, 1, 0, 3, 2, 2, 1, 3, 3, 2, 3,
)


def bit_count(number):
    return number.bit_length() - 1


def flipped(index, bits):
    for bit in bits:
        index = index + (1 - 2 * ((index // (1 << bit)) % 2)) * (1 << bit)
    return index


def subset(bits, number):
    return [bit for place, bit in enumerate(bits) if number >> place & 1]


def greet(me, bits):
    barrier = pltpu.get_barrier_semaphore()
    for bit in bits:
        pl.semaphore_signal(
            barrier, inc=1, device_id={"dev": flipped(me, [bit])}, device_id_type=MESH
        )
    pl.semaphore_wait(barrier, len(bits))


def scatter_steps(me, unit, part_no, order, cols, x_ref, recv, stage, send_sem, recv_sem, block_of):
    k = len(order)
    total = (1 << k) - 1
    first = [total - ((1 << (k - s)) - 1) for s in range(k)]

    def arrived(step, number):
        return pltpu.make_async_remote_copy(
            src_ref=recv.at[first[step] + number, :, cols],
            dst_ref=recv.at[first[step] + number, :, cols],
            send_sem=send_sem.at[part_no, first[step] + number],
            recv_sem=recv_sem.at[part_no, first[step] + number],
            device_id={"dev": flipped(me, [unit + order[step]])},
            device_id_type=MESH,
        )

    copies = []

    def send(step, only=None):
        for number in reversed(range(1 << (k - 1 - step))) if only is None else [only]:
            slot = first[step] + number
            flips = [order[step]] + subset(order[step + 1 :], number)
            block = block_of(flips)
            if step == 0:
                source = x_ref.at[block, :, cols]
            else:
                value = x_ref[block, :, cols].astype(jnp.float32)
                for earlier in range(step):
                    place = (1 << (step - earlier - 1)) + (number << (step - earlier))
                    arrived(earlier, place).wait_recv()
                    value = value + recv[first[earlier] + place, :, cols].astype(jnp.float32)
                spot = slot - first[1]
                stage[spot, :, cols] = value.astype(stage.dtype)
                source = stage.at[spot, :, cols]
            copy = pltpu.make_async_remote_copy(
                src_ref=source,
                dst_ref=recv.at[slot, :, cols],
                send_sem=send_sem.at[part_no, slot],
                recv_sem=recv_sem.at[part_no, slot],
                device_id={"dev": flipped(me, [unit + order[step]])},
                device_id_type=MESH,
            )
            copy.start()
            copies.append(copy)

    def finish(o_ref):
        value = x_ref[block_of([]), :, cols].astype(jnp.float32)
        for earlier in range(k):
            arrived(earlier, 0).wait_recv()
            value = value + recv[first[earlier], :, cols].astype(jnp.float32)
        o_ref[:, cols] = value
        for copy in copies:
            copy.wait_send()

    return send, finish


def scatter_kernel(unit, parts, bits, x_ref, o_ref, recv, stage, send_sem, recv_sem):
    me = lax.axis_index("dev")
    greet(me, [unit + bit for bit in bits])
    rank = me // (1 << unit)
    runs = [
        scatter_steps(
            me, unit, number, order, cols, x_ref, recv, stage, send_sem, recv_sem,
            lambda flips: flipped(rank, flips),
        )
        for number, (order, cols) in enumerate(parts)
    ]
    for step in range(len(bits)):
        for send, _ in runs:
            send(step)
    for _, finish in runs:
        finish(o_ref)


def attend_block(block, length, q_ref, halves, rows):
    heads = q_ref.shape[1] // HEAD_DIM
    picked = pl.ds(pl.multiple_of(block * rows, rows), rows)
    query = jnp.concatenate(
        [q_ref[picked, head * HEAD_DIM : (head + 1) * HEAD_DIM] for head in range(heads)], axis=0
    )
    scale = 1.0 / math.sqrt(HEAD_DIM)
    contract = (((1,), (1,)), ((), ()))
    old = lax.dot_general(query, halves[0, 0], contract, preferred_element_type=jnp.float32) * scale
    new = lax.dot_general(query, halves[1, 0], contract, preferred_element_type=jnp.float32) * scale
    column = lax.broadcasted_iota(jnp.int32, (1, old.shape[1]), 1)
    old = jnp.where(column < length, old, -1e30)
    column = lax.broadcasted_iota(jnp.int32, (rows, new.shape[1]), 1)
    token = lax.broadcasted_iota(jnp.int32, (rows, new.shape[1]), 0) + block * rows
    bias = jnp.where(column <= token, 0.0, -1e30)
    new = new + jnp.concatenate([bias] * heads, axis=0)
    top = jnp.maximum(jnp.max(old, axis=1, keepdims=True), jnp.max(new, axis=1, keepdims=True))
    old = jnp.exp(old - top)
    new = jnp.exp(new - top)
    total = jnp.sum(old, axis=1, keepdims=True) + jnp.sum(new, axis=1, keepdims=True)
    mixed = jnp.dot(old.astype(jnp.bfloat16), halves[0, 1], preferred_element_type=jnp.float32)
    mixed += jnp.dot(new.astype(jnp.bfloat16), halves[1, 1], preferred_element_type=jnp.float32)
    mixed = (mixed / total).astype(jnp.bfloat16)
    return jnp.concatenate(
        [mixed[head * rows : (head + 1) * rows] for head in range(heads)], axis=1
    )


def attention_kernel(
    unit, parts, bits,
    lengths_ref, q_ref, kv_ref, proj_ref, o_ref,
    halves, proj, heads, x, recv, stage,
    send_sem, recv_sem, kv_sem, proj_send, proj_recv, own_sem,
):
    me = lax.axis_index("dev")
    low = list(range(unit))
    mates = [flipped(me, subset(low, number)) for number in range(1, 1 << unit)]
    ranks = [flipped(me, [unit + bit]) for bit in bits]
    barrier = pltpu.get_barrier_semaphore()
    for other in mates + ranks:
        pl.semaphore_signal(barrier, inc=1, device_id={"dev": other}, device_id_type=MESH)
    request = me % (1 << unit)
    rank = me // (1 << unit)
    parity = rank % 2
    depth = proj_ref.shape[0]
    own_rows = pl.ds(pl.multiple_of(request * depth, depth), depth)
    own_half = pltpu.make_async_copy(kv_ref, halves.at[parity], own_sem.at[0])
    own_proj = pltpu.make_async_copy(proj_ref, proj.at[own_rows], own_sem.at[1])
    own_half.start()
    own_proj.start()
    pl.semaphore_wait(barrier, len(mates) + len(ranks))
    kv_copy = pltpu.make_async_remote_copy(
        src_ref=kv_ref,
        dst_ref=halves.at[parity],
        send_sem=kv_sem.at[0],
        recv_sem=kv_sem.at[1],
        device_id={"dev": ranks[0]},
        device_id_type=MESH,
    )
    kv_copy.start()
    proj_copies = []
    for place, other in enumerate(mates):
        copy = pltpu.make_async_remote_copy(
            src_ref=proj_ref,
            dst_ref=proj.at[own_rows],
            send_sem=proj_send.at[place],
            recv_sem=proj_recv.at[place],
            device_id={"dev": other},
            device_id_type=MESH,
        )
        copy.start()
        proj_copies.append(copy)
    own_half.wait()
    kv_copy.wait()

    blocks, rows, width = x.shape
    far = 1 << (len(bits) - 1)
    masks = sorted(range(blocks), key=lambda m: (-bin(m).count("1"), -(m & far), m))
    place_of = {mask: place for place, mask in enumerate(masks)}
    length = lengths_ref[request]
    runs = [
        scatter_steps(
            me, unit, number, order, cols, x, recv, stage, send_sem, recv_sem,
            lambda flips: place_of[sum(1 << bit for bit in flips)],
        )
        for number, (order, cols) in enumerate(parts)
    ]
    half = blocks // 2
    strip = math.gcd(width, 512)
    for group in range(2):
        for spot in range(half):
            mask = masks[group * half + spot]
            block = flipped(rank, subset(bits, mask))
            heads[spot * rows : (spot + 1) * rows, :] = attend_block(
                block, length, q_ref, halves, rows
            )
        if group == 0:
            own_proj.wait()
            for copy in proj_copies:
                copy.wait()
        for start in range(0, width, strip):
            product = jnp.dot(
                heads[...], proj[:, start : start + strip], preferred_element_type=jnp.float32
            ).astype(x.dtype)
            for spot in range(half):
                x[group * half + spot, :, start : start + strip] = product[
                    spot * rows : (spot + 1) * rows
                ]
        for spot in range(half):
            mask = masks[group * half + spot]
            for (send, _), (order, _) in zip(runs, parts):
                if mask >> order[0] & 1:
                    number = sum((mask >> bit & 1) << at for at, bit in enumerate(order[1:]))
                    send(0, number)
    for step in range(1, len(bits)):
        for send, _ in runs:
            send(step)
    for _, finish in runs:
        finish(o_ref)


def attention(lengths, queries, key_values, out_proj, unit, orders, collective_id):
    width = out_proj.shape[1]
    tokens, columns = queries.shape
    bits = sorted(orders[0])
    blocks = 1 << len(bits)
    rows = tokens // blocks
    cut = width * 3 // 4 // 128 * 128
    parts = [(orders[0], pl.ds(0, cut)), (orders[1], pl.ds(cut, width - cut))]
    mates = max((1 << unit) - 1, 1)
    kind = queries.dtype
    whole = pl.BlockSpec(memory_space=pltpu.VMEM)
    return pl.pallas_call(
        functools.partial(attention_kernel, unit, parts, bits),
        out_shape=jax.ShapeDtypeStruct((rows, width), jnp.float32),
        in_specs=[pl.BlockSpec(memory_space=pltpu.SMEM), whole, whole, whole],
        out_specs=whole,
        scratch_shapes=[
            pltpu.VMEM((2,) + key_values.shape, kind),
            pltpu.VMEM((out_proj.shape[0] << unit, width), kind),
            pltpu.VMEM((tokens // 2, columns), kind),
            pltpu.VMEM((blocks, rows, width), kind),
            pltpu.VMEM((blocks - 1, rows, width), kind),
            pltpu.VMEM((max(blocks // 2 - 1, 1), rows, width), kind),
            pltpu.SemaphoreType.DMA((2, blocks - 1)),
            pltpu.SemaphoreType.DMA((2, blocks - 1)),
            pltpu.SemaphoreType.DMA((2,)),
            pltpu.SemaphoreType.DMA((mates,)),
            pltpu.SemaphoreType.DMA((mates,)),
            pltpu.SemaphoreType.DMA((2,)),
        ],
        compiler_params=pltpu.CompilerParams(collective_id=collective_id, has_side_effects=True),
    )(lengths, queries, key_values, out_proj)


def reduce_scatter(x, unit, orders, collective_id):
    blocks, rows, width = x.shape
    bits = sorted(orders[0])
    cut = width * 3 // 4 // 128 * 128
    parts = [(orders[0], pl.ds(0, cut)), (orders[1], pl.ds(cut, width - cut))]
    return pl.pallas_call(
        functools.partial(scatter_kernel, unit, parts, bits),
        out_shape=jax.ShapeDtypeStruct((rows, width), jnp.float32),
        in_specs=[pl.BlockSpec(memory_space=pltpu.VMEM)],
        out_specs=pl.BlockSpec(memory_space=pltpu.VMEM),
        scratch_shapes=[
            pltpu.VMEM((blocks - 1, rows, width), x.dtype),
            pltpu.VMEM((max(blocks // 2 - 1, 1), rows, width), x.dtype),
            pltpu.SemaphoreType.DMA((2, blocks - 1)),
            pltpu.SemaphoreType.DMA((2, blocks - 1)),
        ],
        compiler_params=pltpu.CompilerParams(collective_id=collective_id, has_side_effects=True),
    )(x)


def gather_kernel(parts, bits, x_ref, g_ref, ox_ref, og_ref, send_sem, recv_sem, own_sem):
    me = lax.axis_index("dev")
    greet(me, bits)
    k = len(bits)
    pairs = [(x_ref, ox_ref), (g_ref, og_ref)]
    local = []
    for number, (source, target) in enumerate(pairs):
        copy = pltpu.make_async_copy(source, target.at[me], own_sem.at[number])
        copy.start()
        local.append(copy)
    sent = []

    def forward(part_no, held, step):
        which, order, cols = parts[part_no]
        source, target = pairs[which]
        block = flipped(me, subset(order, held))
        slot = (1 << step) - 1 + held
        copy = pltpu.make_async_remote_copy(
            src_ref=source.at[:, cols] if held == 0 else target.at[block, :, cols],
            dst_ref=target.at[block, :, cols],
            send_sem=send_sem.at[part_no, slot],
            recv_sem=recv_sem.at[part_no, slot],
            device_id={"dev": flipped(me, [order[step]])},
            device_id_type=MESH,
        )
        copy.start()
        sent.append(copy)

    def arrive(part_no, held, step):
        which, order, cols = parts[part_no]
        target = pairs[which][1]
        block = flipped(me, subset(order, held) + [order[step]])
        slot = (1 << step) - 1 + held
        pltpu.make_async_remote_copy(
            src_ref=target.at[block, :, cols],
            dst_ref=target.at[block, :, cols],
            send_sem=send_sem.at[part_no, slot],
            recv_sem=recv_sem.at[part_no, slot],
            device_id={"dev": flipped(me, [order[step]])},
            device_id_type=MESH,
        ).wait_recv()

    for step in range(k):
        for part_no in range(len(parts)):
            forward(part_no, 0, step)
    for step in range(k):
        for held in range(1 << step):
            for part_no in range(len(parts)):
                arrive(part_no, held, step)
                for later in range(step + 1, k):
                    forward(part_no, held + (1 << step), later)
    for copy in local:
        copy.wait()
    for copy in sent:
        copy.wait_send()


def all_gather(x, gates, orders, collective_id):
    rows, width = x.shape
    bits = sorted(orders[0])
    count = 1 << len(bits)
    cut = width * 3 // 4 // 128 * 128
    parts = [
        (1, orders[0], pl.ds(0, gates.shape[1])),
        (0, orders[0], pl.ds(0, cut)),
        (0, orders[1], pl.ds(cut, width - cut)),
    ]
    return pl.pallas_call(
        functools.partial(gather_kernel, parts, bits),
        out_shape=[
            jax.ShapeDtypeStruct((count, rows, width), x.dtype),
            jax.ShapeDtypeStruct((count,) + gates.shape, gates.dtype),
        ],
        in_specs=[pl.BlockSpec(memory_space=pltpu.VMEM)] * 2,
        out_specs=[pl.BlockSpec(memory_space=pltpu.VMEM)] * 2,
        scratch_shapes=[
            pltpu.SemaphoreType.DMA((3, count - 1)),
            pltpu.SemaphoreType.DMA((3, count - 1)),
            pltpu.SemaphoreType.DMA((2,)),
        ],
        compiler_params=pltpu.CompilerParams(collective_id=collective_id, has_side_effects=True),
    )(x, gates)


def plain_order(counts, lag):
    entries = [(step + lag * k, k) for k, count in enumerate(counts) for step in range(count)]
    return [k for _, k in sorted(entries)]


def moe_fits(devices, rows, width, hidden):
    if devices < 8 or rows % (16 * CHUNKS):
        return False
    weights = 3 * width * hidden
    tokens = devices * rows * width
    return 2 * (weights + 4 * tokens) < 48 * 2**20


def moe_kernel(
    line, ag_kinds,
    att_ref, res_ref, gain_ref, router_ref, ids_ref, gu_hbm, dn_hbm, o_ref,
    gath, gu, dn, act, made, mrecv, part, yrecv, half, zrecv, held,
    w_sem, ag_send, ag_recv, m_send, m_recv, y_send, y_recv, z_send, z_recv,
):
    me = lax.axis_index("dev")
    z, y, c = me // 4, (me // 2) % 2, me % 2
    chunks, total, padded = gath.shape
    rows, width = o_ref.shape
    R = rows // chunks
    hidden = dn.shape[0]
    experts = router_ref.shape[0]
    dest = [me + 4, me - 4, me + 2 - 4 * y, me + 1 - 2 * c]
    allowed = [z + 1 < line, z > 0, None, None]
    RIGHT, LEFT, YMATE, MATE = range(4)

    def guarded(cond, body):
        if cond is None:
            body()
        else:
            pl.when(cond)(body)

    def both(*conds):
        conds = [cond for cond in conds if cond is not None]
        if not conds:
            return None
        return functools.reduce(jnp.logical_and, conds)

    copies = [
        pltpu.make_async_copy(gu_hbm.at[0], gu, w_sem.at[0]),
        pltpu.make_async_copy(dn_hbm.at[0], dn, w_sem.at[1]),
    ]
    for copy in copies:
        copy.start()
    barrier = pltpu.get_barrier_semaphore()
    offsets = [sign * step for step in range(line - 1, 0, -1) for sign in (1, -1)]

    def exists(offset):
        if offset == 0:
            return None
        return z + offset >= 0 if offset < 0 else z + offset < line

    def greet_one(other):
        pl.semaphore_signal(barrier, inc=1, device_id={"dev": other}, device_id_type=MESH)

    greet_one(dest[YMATE])
    greet_one(dest[MATE])
    for offset in offsets:
        pl.when(exists(offset))(lambda offset=offset: greet_one(me + 4 * offset))

    stream = (res_ref[...].astype(jnp.float32) + att_ref[...]).astype(jnp.bfloat16)
    values = stream.astype(jnp.float32)
    held[...] = values
    scale = lax.rsqrt(jnp.mean(values * values, axis=-1, keepdims=True) + EPSILON)
    normed = (values * scale * gain_ref[...].astype(jnp.float32).reshape(1, width)).astype(jnp.bfloat16)
    logits = lax.dot_general(
        router_ref[...], normed, (((1,), (1,)), ((), ())), preferred_element_type=jnp.float32
    )
    number = lax.broadcasted_iota(jnp.int32, (experts, rows), 0)
    named = ids_ref[0:1, :] == number
    for place in range(1, ids_ref.shape[0]):
        named = jnp.logical_or(named, ids_ref[place : place + 1, :] == number)
    raised = jnp.where(named, jnp.exp(logits), 0.0)
    gates = raised / jnp.sum(raised, axis=0, keepdims=True)
    high = gates.astype(jnp.bfloat16).astype(jnp.float32)
    low = gates - high
    spare = jnp.zeros((padded - width - 2 * experts, rows), jnp.float32)
    extra = jnp.concatenate([high, low, spare], axis=0).T.astype(jnp.bfloat16)

    def spot(core, column, place):
        return pl.multiple_of(((core * 2 + column) * line + place) * R, R)

    mine = pl.ds(spot(c, y, z), R)
    for k in range(chunks):
        gath[k, mine, 0:width] = normed[k * R : (k + 1) * R]
        gath[k, mine, width:padded] = extra[k * R : (k + 1) * R]

    pl.semaphore_wait(barrier, line + 1)

    span = 2 * line - 1
    started = []

    def label(side, offset):
        return side * span + offset + line - 1

    def slab(k, side, offset):
        column = y if side == 0 else 1 - y
        return gath.at[k, pl.ds(spot(c, column, z + offset), R), :]

    def ag_copy(k, side, offset, way):
        if way == RIGHT:
            landing = label(side, offset - 1)
        elif way == LEFT:
            landing = label(side, offset + 1)
        elif way == YMATE:
            landing = label(1 - side, offset)
        else:
            landing = 2 * span + label(side, offset)
        where = slab(k, side, offset)
        return pltpu.make_async_remote_copy(
            src_ref=where, dst_ref=where,
            send_sem=ag_send.at[k, label(side, offset), way],
            recv_sem=ag_recv.at[k, landing],
            device_id={"dev": dest[way]}, device_id_type=MESH,
        )

    def ag_ways(k, side, offset):
        kind = ag_kinds[k]
        ways = []
        if kind == 0:
            if side == 0:
                if offset <= 0 and offset > 1 - line:
                    ways.append(RIGHT)
                if offset >= 0 and offset < line - 1:
                    ways.append(LEFT)
                ways.append(YMATE)
        else:
            if side == 0 and offset == 0:
                ways.append(YMATE)
            if offset <= 0 and offset > 1 - line:
                ways.append(RIGHT)
            if offset >= 0 and offset < line - 1:
                ways.append(LEFT)
        ways.append(MATE)
        return ways

    def ag_step(k, side, offset):
        def body():
            if side or offset:
                arrived = slab(k, side, offset)
                pltpu.make_async_remote_copy(
                    src_ref=arrived, dst_ref=arrived,
                    send_sem=ag_send.at[k, label(side, offset), MATE],
                    recv_sem=ag_recv.at[k, label(side, offset)],
                    device_id={"dev": dest[MATE]}, device_id_type=MESH,
                ).wait_recv()
            for way in ag_ways(k, side, offset):
                copy = ag_copy(k, side, offset, way)
                guarded(allowed[way], copy.start)

        guarded(exists(offset), body)
        for way in ag_ways(k, side, offset):
            started.append(
                (
                    lambda way=way: both(exists(offset), allowed[way]),
                    lambda way=way: ag_copy(k, side, offset, way),
                )
            )

    def ag_stage(k, stage):
        if stage == 0:
            ag_step(k, 0, 0)
            return
        if stage < line:
            ag_step(k, 0, -stage)
            ag_step(k, 0, stage)
        if stage == 1:
            ag_step(k, 1, 0)
        else:
            ag_step(k, 1, 1 - stage)
            ag_step(k, 1, stage - 1)

    def mate_wait(k):
        for side in range(2):
            for offset in range(1 - line, line):
                column = y if side == 0 else 1 - y

                def body(side=side, offset=offset, column=column):
                    where = gath.at[k, pl.ds(spot(1 - c, column, z + offset), R), :]
                    pltpu.make_async_remote_copy(
                        src_ref=where, dst_ref=where,
                        send_sem=ag_send.at[k, label(side, offset), MATE],
                        recv_sem=ag_recv.at[k, 2 * span + label(side, offset)],
                        device_id={"dev": dest[MATE]}, device_id_type=MESH,
                    ).wait_recv()

                guarded(exists(offset), body)

    core_rows = total // 2
    strip = math.gcd(hidden, 256)

    wide = math.gcd(width, 512)

    def rise(k, start):
        if start == 0:
            if k == 0:
                for copy in copies:
                    copy.wait()
            mate_wait(k)
        x = gath[k, :, 0:width]
        if True:
            gate = jnp.dot(x, gu[:, start : start + strip], preferred_element_type=jnp.float32)
            up = jnp.dot(
                x, gu[:, hidden + start : hidden + start + strip],
                preferred_element_type=jnp.float32,
            )
            act[:, start : start + strip] = (gate / (1.0 + jnp.exp(-gate)) * up).astype(act.dtype)

    def fall(k, start):
        tail = gath[k, :, width:padded].astype(jnp.float32)
        lanes = lax.broadcasted_iota(jnp.int32, tail.shape, 1)
        chosen = jnp.logical_or(lanes == me, lanes == me + experts)
        weight = jnp.sum(jnp.where(chosen, tail, 0.0), axis=1, keepdims=True)
        if True:
            produced = jnp.dot(
                act[...], dn[:, start : start + wide], preferred_element_type=jnp.float32
            )
            made[k, :, start : start + wide] = (weight * produced).astype(made.dtype)
        if start + wide == width:
            mate_copy(k).start()
            started.append((lambda: None, lambda: mate_copy(k)))

    def mate_copy(k):
        theirs = pl.ds(pl.multiple_of((1 - c) * core_rows, core_rows), core_rows)
        return pltpu.make_async_remote_copy(
            src_ref=made.at[k, theirs, :], dst_ref=mrecv.at[k],
            send_sem=m_send.at[k], recv_sem=m_recv.at[k],
            device_id={"dev": dest[MATE]}, device_id_type=MESH,
        )

    def y_copy(k):
        return pltpu.make_async_remote_copy(
            src_ref=part.at[k, 1 - y], dst_ref=yrecv.at[k],
            send_sem=y_send.at[k], recv_sem=y_recv.at[k],
            device_id={"dev": dest[YMATE]}, device_id_type=MESH,
        )

    def z_copy(k, offset):
        target = jnp.clip(z + offset, 0, line - 1)
        return pltpu.make_async_remote_copy(
            src_ref=half.at[k, target], dst_ref=zrecv.at[k, line - 1 - offset],
            send_sem=z_send.at[k, line - 1 + offset], recv_sem=z_recv.at[k, line - 1 - offset],
            device_id={"dev": me + 4 * (target - z)}, device_id_type=MESH,
        )

    def z_arrived(k, offset):
        where = zrecv.at[k, line - 1 + offset]
        return pltpu.make_async_remote_copy(
            src_ref=where, dst_ref=where,
            send_sem=z_send.at[k, line - 1 + offset], recv_sem=z_recv.at[k, line - 1 + offset],
            device_id={"dev": dest[MATE]}, device_id_type=MESH,
        )

    def merge(k):
        mate_copy(k).wait_recv()
        for column in range(2):
            for place in range(line):
                at = column * line + place
                ours = pl.ds(pl.multiple_of(c * core_rows + at * R, R), R)
                part[k, column, place] = (
                    made[k, ours, :].astype(jnp.float32)
                    + mrecv[k, at * R : (at + 1) * R, :].astype(jnp.float32)
                ).astype(part.dtype)
        y_copy(k).start()
        started.append((lambda: None, lambda: y_copy(k)))

    def y_merge(k):
        y_copy(k).wait_recv()
        for place in range(line):
            half[k, place] = (
                part[k, y, place].astype(jnp.float32) + yrecv[k, place].astype(jnp.float32)
            ).astype(half.dtype)

    def z_scatter(k):
        for offset in offsets:
            pl.when(exists(offset))(lambda offset=offset: z_copy(k, offset).start())
            started.append(
                (lambda offset=offset: exists(offset), lambda offset=offset: z_copy(k, offset))
            )

    def finish(k):
        where = pl.ds(k * R, R)
        held[where, :] = held[where, :] + half[k, z].astype(jnp.float32)
        for offset in reversed(offsets):

            def add(offset=offset):
                z_arrived(k, offset).wait_recv()
                held[where, :] = held[where, :] + zrecv[k, line - 1 + offset].astype(jnp.float32)

            pl.when(exists(offset))(add)
        o_ref[where, :] = held[where, :].astype(o_ref.dtype)

    rs_stages = [merge, y_merge, z_scatter, finish]
    pieces = [functools.partial(rise, start=start) for start in range(0, hidden, strip)]
    pieces += [functools.partial(fall, start=start) for start in range(0, width, wide)]
    queues = []
    for k in range(chunks):
        steps = [functools.partial(ag_stage, k, stage) for stage in range(line + 1)]
        steps += [functools.partial(piece, k) for piece in pieces]
        steps += [functools.partial(step, k) for step in rs_stages]
        queues.append(steps)
    order = ORDER
    if [order.count(k) for k in range(chunks)] != [len(steps) for steps in queues]:
        order = plain_order([len(steps) for steps in queues], line + 1 + len(pieces) // 2)
    for k in order:
        queues[k].pop(0)()
    for cond, copy in started:
        guarded(cond(), lambda copy=copy: copy().wait_send())


def moe(attended, residual, gain, router, ids, gate_up, down, collective_id):
    devices = lax.axis_size("dev")
    rows, width = residual.shape
    hidden = down.shape[1]
    experts = router.shape[0]
    line = devices // 4
    padded = width + -(-2 * experts // 128) * 128
    R = rows // CHUNKS
    kind = residual.dtype
    span = 2 * line - 1
    vmem = pl.BlockSpec(memory_space=pltpu.VMEM)
    hbm = pl.BlockSpec(memory_space=pl.ANY)
    dma = pltpu.SemaphoreType.DMA
    total = devices * R
    return pl.pallas_call(
        functools.partial(moe_kernel, line, AG_KINDS),
        out_shape=jax.ShapeDtypeStruct((rows, width), kind),
        in_specs=[vmem] * 5 + [hbm] * 2,
        out_specs=vmem,
        scratch_shapes=[
            pltpu.VMEM((CHUNKS, total, padded), kind),
            pltpu.VMEM(gate_up.shape[1:], kind),
            pltpu.VMEM(down.shape[1:], kind),
            pltpu.VMEM((total, hidden), kind),
            pltpu.VMEM((CHUNKS, total, width), kind),
            pltpu.VMEM((CHUNKS, total // 2, width), kind),
            pltpu.VMEM((CHUNKS, 2, line, R, width), kind),
            pltpu.VMEM((CHUNKS, line, R, width), kind),
            pltpu.VMEM((CHUNKS, line, R, width), kind),
            pltpu.VMEM((CHUNKS, span, R, width), kind),
            pltpu.VMEM((rows, width), jnp.float32),
            dma((2,)),
            dma((CHUNKS, 2 * span, 4)),
            dma((CHUNKS, 4 * span)),
            dma((CHUNKS,)),
            dma((CHUNKS,)),
            dma((CHUNKS,)),
            dma((CHUNKS,)),
            dma((CHUNKS, span)),
            dma((CHUNKS, span)),
        ],
        compiler_params=pltpu.CompilerParams(collective_id=collective_id, has_side_effects=True),
    )(attended, residual, gain, router, ids, gate_up, down)


def swapped(order, one, two):
    order = list(order)
    order[one], order[two] = order[two], order[one]
    return order


def per_device(
    queries,
    key_values,
    lengths,
    out_proj,
    residual,
    norm_gain,
    router,
    expert_ids,
    expert_gate_up,
    expert_down,
):
    devices = lax.axis_size("dev")
    my_index = lax.axis_index("dev")
    width = residual.shape[-1]
    requests_n = devices // GROUP
    low_bits = bit_count(requests_n)
    near = list(range(bit_count(GROUP)))
    attended = attention(
        lengths, queries[0], key_values[:, 0], out_proj, low_bits, [near, swapped(near, 0, 1)], 1
    )
    if moe_fits(devices, TOK_DEV, width, FF):
        return moe(
            attended, residual[0], norm_gain, router.T, expert_ids[0].T,
            expert_gate_up, expert_down, 2,
        )[None]
    stream = (residual[0].astype(jnp.float32) + attended).astype(jnp.bfloat16)
    values = stream.astype(jnp.float32)
    normed = (
        values
        * lax.rsqrt(jnp.mean(values * values, axis=-1, keepdims=True) + EPSILON)
        * norm_gain.astype(jnp.float32)
    ).astype(jnp.bfloat16)
    logits = jnp.dot(normed, router, preferred_element_type=jnp.float32)
    experts_n = router.shape[1]
    token_ids = expert_ids[0]
    named = jnp.any(token_ids[..., None] == jnp.arange(experts_n, dtype=jnp.int32), axis=1)
    raised_gate = jnp.where(named, jnp.exp(logits), 0.0)
    gates = raised_gate / jnp.sum(raised_gate, axis=-1, keepdims=True)
    lanes = -(-TOK_DEV // 128) * 128
    gates = jnp.pad(gates.T, ((0, 0), (0, lanes - TOK_DEV)))
    every = list(range(bit_count(devices)))
    far = every[::-1]
    count = len(far)
    rows_all, gates_all = all_gather(normed, gates, [far, swapped(far, count - 3, count - 2)], 2)
    my_gates = lax.dynamic_index_in_dim(gates_all, my_index, 1, keepdims=False)[:, :TOK_DEV]
    flat_rows = rows_all.reshape(devices * TOK_DEV, width)
    projected = jnp.dot(flat_rows, expert_gate_up[0], preferred_element_type=jnp.float32)
    activation = (jax.nn.silu(projected[:, :FF]) * projected[:, FF:]).astype(jnp.bfloat16)
    produced = jnp.dot(activation, expert_down[0], preferred_element_type=jnp.float32)
    weighted = (my_gates.reshape(-1, 1) * produced).astype(jnp.bfloat16)
    weighted = weighted.reshape(devices, TOK_DEV, width)
    combined = reduce_scatter(weighted, 0, [every, swapped(every, 1, 2)], 3)
    return (values + combined).astype(jnp.bfloat16)[None]


def solution(mesh):
    return jax.shard_map(
        per_device,
        mesh=mesh,
        in_specs=(
            P(("groups", "dev"), None, None),
            P(None, ("groups", "dev"), None, None),
            P("groups"),
            P("dev", None),
            P(("groups", "dev"), None, None),
            P(),
            P(),
            P(("groups", "dev"), None, None),
            P("dev", None, None),
            P("dev", None, None),
        ),
        out_specs=P(("groups", "dev"), None, None),
        check_vma=False,
    )
```

```python
import functools
import math

import jax
import jax.numpy as jnp
from jax import lax
from jax.experimental import pallas as pl
from jax.experimental.pallas import tpu as pltpu
from jax.sharding import PartitionSpec as P

HEAD_DIM = 128
FF = 768
TOK_DEV = 64
GROUP = 8
EPSILON = 1e-06
MESH = pl.DeviceIdType.MESH
CHUNKS = 4
ATTENTION_GROUPS = 8
GATHER_SHARE = 6
SCATTER_SHARE = 2
ORDER = (
    0, 1, 0, 1, 0, 3, 0, 1, 2, 0, 3, 0, 1, 0, 0, 0, 2, 0, 1, 0, 0, 3, 1, 1,
    3, 2, 0, 1, 3, 1, 1, 1, 1, 2, 3, 3, 3, 3, 3, 3, 3, 1, 0, 2, 3, 2, 2, 2,
    2, 2, 2, 2, 1, 2, 0, 3, 2, 3, 1, 2,
)


def bit_count(number):
    return number.bit_length() - 1


def flipped(index, bits):
    for bit in bits:
        index = index + (1 - 2 * ((index // (1 << bit)) % 2)) * (1 << bit)
    return index


def subset(bits, number):
    return [bit for place, bit in enumerate(bits) if number >> place & 1]


def greet(me, bits):
    barrier = pltpu.get_barrier_semaphore()
    for bit in bits:
        pl.semaphore_signal(
            barrier, inc=1, device_id={"dev": flipped(me, [bit])}, device_id_type=MESH
        )
    pl.semaphore_wait(barrier, len(bits))


def scatter_steps(me, unit, part_no, order, cols, x_ref, recv, stage, send_sem, recv_sem, block_of):
    k = len(order)
    total = (1 << k) - 1
    first = [total - ((1 << (k - s)) - 1) for s in range(k)]

    def arrived(step, number):
        return pltpu.make_async_remote_copy(
            src_ref=recv.at[first[step] + number, :, cols],
            dst_ref=recv.at[first[step] + number, :, cols],
            send_sem=send_sem.at[part_no, first[step] + number],
            recv_sem=recv_sem.at[part_no, first[step] + number],
            device_id={"dev": flipped(me, [unit + order[step]])},
            device_id_type=MESH,
        )

    copies = []

    def send(step, only=None):
        for number in reversed(range(1 << (k - 1 - step))) if only is None else [only]:
            slot = first[step] + number
            flips = [order[step]] + subset(order[step + 1 :], number)
            block = block_of(flips)
            if step == 0:
                source = x_ref.at[block, :, cols]
            else:
                value = x_ref[block, :, cols].astype(jnp.float32)
                for earlier in range(step):
                    place = (1 << (step - earlier - 1)) + (number << (step - earlier))
                    arrived(earlier, place).wait_recv()
                    value = value + recv[first[earlier] + place, :, cols].astype(jnp.float32)
                spot = slot - first[1]
                stage[spot, :, cols] = value.astype(stage.dtype)
                source = stage.at[spot, :, cols]
            copy = pltpu.make_async_remote_copy(
                src_ref=source,
                dst_ref=recv.at[slot, :, cols],
                send_sem=send_sem.at[part_no, slot],
                recv_sem=recv_sem.at[part_no, slot],
                device_id={"dev": flipped(me, [unit + order[step]])},
                device_id_type=MESH,
            )
            copy.start()
            copies.append(copy)

    def finish(o_ref):
        value = x_ref[block_of([]), :, cols].astype(jnp.float32)
        for earlier in range(k):
            arrived(earlier, 0).wait_recv()
            value = value + recv[first[earlier], :, cols].astype(jnp.float32)
        o_ref[:, cols] = value
        for copy in copies:
            copy.wait_send()

    return send, finish


def scatter_kernel(unit, parts, bits, x_ref, o_ref, recv, stage, send_sem, recv_sem):
    me = lax.axis_index("dev")
    greet(me, [unit + bit for bit in bits])
    rank = me // (1 << unit)
    runs = [
        scatter_steps(
            me, unit, number, order, cols, x_ref, recv, stage, send_sem, recv_sem,
            lambda flips: flipped(rank, flips),
        )
        for number, (order, cols) in enumerate(parts)
    ]
    for step in range(len(bits)):
        for send, _ in runs:
            send(step)
    for _, finish in runs:
        finish(o_ref)


def attend_block(block, length, q_ref, halves, rows, values_ready=None):
    heads = q_ref.shape[1] // HEAD_DIM
    picked = pl.ds(pl.multiple_of(block * rows, rows), rows)
    query = jnp.concatenate(
        [q_ref[picked, head * HEAD_DIM : (head + 1) * HEAD_DIM] for head in range(heads)], axis=0
    )
    scale = 1.0 / math.sqrt(HEAD_DIM)
    contract = (((1,), (1,)), ((), ()))
    old = lax.dot_general(query, halves[0, 0], contract, preferred_element_type=jnp.float32) * scale
    new = lax.dot_general(query, halves[1, 0], contract, preferred_element_type=jnp.float32) * scale
    column = lax.broadcasted_iota(jnp.int32, (1, old.shape[1]), 1)
    old = jnp.where(column < length, old, -1e30)
    column = lax.broadcasted_iota(jnp.int32, (rows, new.shape[1]), 1)
    token = lax.broadcasted_iota(jnp.int32, (rows, new.shape[1]), 0) + block * rows
    bias = jnp.where(column <= token, 0.0, -1e30)
    new = new + jnp.concatenate([bias] * heads, axis=0)
    top = jnp.maximum(jnp.max(old, axis=1, keepdims=True), jnp.max(new, axis=1, keepdims=True))
    old = jnp.exp(old - top)
    new = jnp.exp(new - top)
    total = jnp.sum(old, axis=1, keepdims=True) + jnp.sum(new, axis=1, keepdims=True)
    if values_ready is not None:
        values_ready()
    mixed = jnp.dot(old.astype(jnp.bfloat16), halves[0, 1], preferred_element_type=jnp.float32)
    mixed += jnp.dot(new.astype(jnp.bfloat16), halves[1, 1], preferred_element_type=jnp.float32)
    mixed = (mixed / total).astype(jnp.bfloat16)
    return jnp.concatenate(
        [mixed[head * rows : (head + 1) * rows] for head in range(heads)], axis=1
    )


def attention_kernel(
    unit, parts, bits,
    lengths_ref, q_ref, kv_ref, proj_ref, o_ref,
    halves, proj, heads, x, recv, stage,
    send_sem, recv_sem, kv_sem, proj_send, proj_recv, own_sem,
):
    me = lax.axis_index("dev")
    low = list(range(unit))
    mates = [flipped(me, subset(low, number)) for number in range(1, 1 << unit)]
    ranks = [flipped(me, [unit + bit]) for bit in bits]
    barrier = pltpu.get_barrier_semaphore()
    for other in mates + ranks:
        pl.semaphore_signal(barrier, inc=1, device_id={"dev": other}, device_id_type=MESH)
    request = me % (1 << unit)
    rank = me // (1 << unit)
    parity = rank % 2
    depth = proj_ref.shape[0]
    own_rows = pl.ds(pl.multiple_of(request * depth, depth), depth)
    own_half = pltpu.make_async_copy(kv_ref, halves.at[parity], own_sem.at[0])
    own_proj = pltpu.make_async_copy(proj_ref, proj.at[own_rows], own_sem.at[1])
    own_half.start()
    own_proj.start()
    pl.semaphore_wait(barrier, len(mates) + len(ranks))
    kv_copies = [
        pltpu.make_async_remote_copy(
            src_ref=kv_ref.at[place],
            dst_ref=halves.at[parity, place],
            send_sem=kv_sem.at[place],
            recv_sem=kv_sem.at[2 + place],
            device_id={"dev": ranks[0]},
            device_id_type=MESH,
        )
        for place in range(2)
    ]
    for copy in kv_copies:
        copy.start()
    proj_copies = []
    for place, other in enumerate(mates):
        copy = pltpu.make_async_remote_copy(
            src_ref=proj_ref,
            dst_ref=proj.at[own_rows],
            send_sem=proj_send.at[place],
            recv_sem=proj_recv.at[place],
            device_id={"dev": other},
            device_id_type=MESH,
        )
        copy.start()
        proj_copies.append(copy)
    own_half.wait()
    kv_copies[0].wait()

    blocks, rows, width = x.shape
    far = 1 << (len(bits) - 1)
    masks = sorted(range(blocks), key=lambda m: (-bin(m).count("1"), -(m & far), m))
    place_of = {mask: place for place, mask in enumerate(masks)}
    length = lengths_ref[request]
    runs = [
        scatter_steps(
            me, unit, number, order, cols, x, recv, stage, send_sem, recv_sem,
            lambda flips: place_of[sum(1 << bit for bit in flips)],
        )
        for number, (order, cols) in enumerate(parts)
    ]
    groups = min(ATTENTION_GROUPS, blocks)
    half = blocks // groups
    strip = math.gcd(width, 512)
    for group in range(groups):
        for spot in range(half):
            mask = masks[group * half + spot]
            block = flipped(rank, subset(bits, mask))
            heads[spot * rows : (spot + 1) * rows, :] = attend_block(
                block, length, q_ref, halves, rows,
                kv_copies[1].wait if group == 0 and spot == 0 else None,
            )
        if group == 0:
            own_proj.wait()
            for copy in proj_copies:
                copy.wait()
        for start in range(0, width, strip):
            product = jnp.dot(
                heads[...], proj[:, start : start + strip], preferred_element_type=jnp.float32
            ).astype(x.dtype)
            for spot in range(half):
                x[group * half + spot, :, start : start + strip] = product[
                    spot * rows : (spot + 1) * rows
                ]
        for spot in range(half):
            mask = masks[group * half + spot]
            for (send, _), (order, _) in zip(runs, parts):
                if mask >> order[0] & 1:
                    number = sum((mask >> bit & 1) << at for at, bit in enumerate(order[1:]))
                    send(0, number)
    for step in range(1, len(bits)):
        for send, _ in runs:
            send(step)
    for _, finish in runs:
        finish(o_ref)


def attention(lengths, queries, key_values, out_proj, unit, orders, collective_id):
    width = out_proj.shape[1]
    tokens, columns = queries.shape
    bits = sorted(orders[0])
    blocks = 1 << len(bits)
    rows = tokens // blocks
    cut = width * 13 // 16 // 128 * 128
    parts = [(orders[0], pl.ds(0, cut)), (orders[1], pl.ds(cut, width - cut))]
    mates = max((1 << unit) - 1, 1)
    kind = queries.dtype
    whole = pl.BlockSpec(memory_space=pltpu.VMEM)
    return pl.pallas_call(
        functools.partial(attention_kernel, unit, parts, bits),
        out_shape=jax.ShapeDtypeStruct((rows, width), jnp.float32),
        in_specs=[pl.BlockSpec(memory_space=pltpu.SMEM), whole, whole, whole],
        out_specs=whole,
        scratch_shapes=[
            pltpu.VMEM((2,) + key_values.shape, kind),
            pltpu.VMEM((out_proj.shape[0] << unit, width), kind),
            pltpu.VMEM((tokens // min(ATTENTION_GROUPS, blocks), columns), kind),
            pltpu.VMEM((blocks, rows, width), kind),
            pltpu.VMEM((blocks - 1, rows, width), kind),
            pltpu.VMEM((max(blocks // 2 - 1, 1), rows, width), kind),
            pltpu.SemaphoreType.DMA((2, blocks - 1)),
            pltpu.SemaphoreType.DMA((2, blocks - 1)),
            pltpu.SemaphoreType.DMA((4,)),
            pltpu.SemaphoreType.DMA((mates,)),
            pltpu.SemaphoreType.DMA((mates,)),
            pltpu.SemaphoreType.DMA((2,)),
        ],
        compiler_params=pltpu.CompilerParams(collective_id=collective_id, has_side_effects=True),
    )(lengths, queries, key_values, out_proj)


def reduce_scatter(x, unit, orders, collective_id):
    blocks, rows, width = x.shape
    bits = sorted(orders[0])
    cut = width * 3 // 4 // 128 * 128
    parts = [(orders[0], pl.ds(0, cut)), (orders[1], pl.ds(cut, width - cut))]
    return pl.pallas_call(
        functools.partial(scatter_kernel, unit, parts, bits),
        out_shape=jax.ShapeDtypeStruct((rows, width), jnp.float32),
        in_specs=[pl.BlockSpec(memory_space=pltpu.VMEM)],
        out_specs=pl.BlockSpec(memory_space=pltpu.VMEM),
        scratch_shapes=[
            pltpu.VMEM((blocks - 1, rows, width), x.dtype),
            pltpu.VMEM((max(blocks // 2 - 1, 1), rows, width), x.dtype),
            pltpu.SemaphoreType.DMA((2, blocks - 1)),
            pltpu.SemaphoreType.DMA((2, blocks - 1)),
        ],
        compiler_params=pltpu.CompilerParams(collective_id=collective_id, has_side_effects=True),
    )(x)


def gather_kernel(parts, bits, x_ref, g_ref, ox_ref, og_ref, send_sem, recv_sem, own_sem):
    me = lax.axis_index("dev")
    greet(me, bits)
    k = len(bits)
    pairs = [(x_ref, ox_ref), (g_ref, og_ref)]
    local = []
    for number, (source, target) in enumerate(pairs):
        copy = pltpu.make_async_copy(source, target.at[me], own_sem.at[number])
        copy.start()
        local.append(copy)
    sent = []

    def forward(part_no, held, step):
        which, order, cols = parts[part_no]
        source, target = pairs[which]
        block = flipped(me, subset(order, held))
        slot = (1 << step) - 1 + held
        copy = pltpu.make_async_remote_copy(
            src_ref=source.at[:, cols] if held == 0 else target.at[block, :, cols],
            dst_ref=target.at[block, :, cols],
            send_sem=send_sem.at[part_no, slot],
            recv_sem=recv_sem.at[part_no, slot],
            device_id={"dev": flipped(me, [order[step]])},
            device_id_type=MESH,
        )
        copy.start()
        sent.append(copy)

    def arrive(part_no, held, step):
        which, order, cols = parts[part_no]
        target = pairs[which][1]
        block = flipped(me, subset(order, held) + [order[step]])
        slot = (1 << step) - 1 + held
        pltpu.make_async_remote_copy(
            src_ref=target.at[block, :, cols],
            dst_ref=target.at[block, :, cols],
            send_sem=send_sem.at[part_no, slot],
            recv_sem=recv_sem.at[part_no, slot],
            device_id={"dev": flipped(me, [order[step]])},
            device_id_type=MESH,
        ).wait_recv()

    for step in range(k):
        for part_no in range(len(parts)):
            forward(part_no, 0, step)
    for step in range(k):
        for held in range(1 << step):
            for part_no in range(len(parts)):
                arrive(part_no, held, step)
                for later in range(step + 1, k):
                    forward(part_no, held + (1 << step), later)
    for copy in local:
        copy.wait()
    for copy in sent:
        copy.wait_send()


def all_gather(x, gates, orders, collective_id):
    rows, width = x.shape
    bits = sorted(orders[0])
    count = 1 << len(bits)
    cut = width * 3 // 4 // 128 * 128
    parts = [
        (1, orders[0], pl.ds(0, gates.shape[1])),
        (0, orders[0], pl.ds(0, cut)),
        (0, orders[1], pl.ds(cut, width - cut)),
    ]
    return pl.pallas_call(
        functools.partial(gather_kernel, parts, bits),
        out_shape=[
            jax.ShapeDtypeStruct((count, rows, width), x.dtype),
            jax.ShapeDtypeStruct((count,) + gates.shape, gates.dtype),
        ],
        in_specs=[pl.BlockSpec(memory_space=pltpu.VMEM)] * 2,
        out_specs=[pl.BlockSpec(memory_space=pltpu.VMEM)] * 2,
        scratch_shapes=[
            pltpu.SemaphoreType.DMA((3, count - 1)),
            pltpu.SemaphoreType.DMA((3, count - 1)),
            pltpu.SemaphoreType.DMA((2,)),
        ],
        compiler_params=pltpu.CompilerParams(collective_id=collective_id, has_side_effects=True),
    )(x, gates)


def plain_order(counts, lag):
    entries = [(step + lag * k, k) for k, count in enumerate(counts) for step in range(count)]
    return [k for _, k in sorted(entries)]


def moe_fits(devices, rows, width, hidden):
    if devices < 8 or rows % (16 * CHUNKS):
        return False
    weights = 3 * width * hidden
    tokens = devices * rows * width
    return 2 * (weights + 4 * tokens) < 48 * 2**20


def moe_kernel(
    line, gather_cut, scatter_cut,
    att_ref, res_ref, gain_ref, router_ref, ids_ref, gu_hbm, dn_hbm, o_ref,
    gath, gu, dn, act, made, mrecv, part, yrecv, half, zrecv, held, ready, ylate, zearly, cross,
    w_sem, ag_send, ag_recv, pass_send, pass_recv, m_send, m_recv, y_send, y_recv, z_send, z_recv,
):
    me = lax.axis_index("dev")
    z, y, c = me // 4, (me // 2) % 2, me % 2
    chunks, total, padded = gath.shape
    rows, width = o_ref.shape
    R = rows // chunks
    hidden = dn.shape[0]
    experts = router_ref.shape[0]
    dest = [me + 4, me - 4, me + 2 - 4 * y, me + 1 - 2 * c]
    allowed = [z + 1 < line, z > 0, None, None]
    RIGHT, LEFT, YMATE, MATE = range(4)

    def guarded(cond, body):
        if cond is None:
            body()
        else:
            pl.when(cond)(body)

    def both(*conds):
        conds = [cond for cond in conds if cond is not None]
        if not conds:
            return None
        return functools.reduce(jnp.logical_and, conds)

    copies = [
        pltpu.make_async_copy(gu_hbm.at[0], gu, w_sem.at[0]),
        pltpu.make_async_copy(dn_hbm.at[0], dn, w_sem.at[1]),
    ]
    for copy in copies:
        copy.start()
    barrier = pltpu.get_barrier_semaphore()
    offsets = [sign * step for step in range(line - 1, 0, -1) for sign in (1, -1)]

    def exists(offset):
        if offset == 0:
            return None
        return z + offset >= 0 if offset < 0 else z + offset < line

    def greet_one(other):
        pl.semaphore_signal(barrier, inc=1, device_id={"dev": other}, device_id_type=MESH)

    greet_one(dest[YMATE])
    greet_one(dest[MATE])
    for offset in offsets:
        pl.when(exists(offset))(lambda offset=offset: greet_one(me + 4 * offset))

    stream = (res_ref[...].astype(jnp.float32) + att_ref[...]).astype(jnp.bfloat16)
    values = stream.astype(jnp.float32)
    held[...] = values
    scale = lax.rsqrt(jnp.mean(values * values, axis=-1, keepdims=True) + EPSILON)
    normed = (values * scale * gain_ref[...].astype(jnp.float32).reshape(1, width)).astype(jnp.bfloat16)
    logits = lax.dot_general(
        router_ref[...], normed, (((1,), (1,)), ((), ())), preferred_element_type=jnp.float32
    )
    number = lax.broadcasted_iota(jnp.int32, (experts, rows), 0)
    named = ids_ref[0:1, :] == number
    for place in range(1, ids_ref.shape[0]):
        named = jnp.logical_or(named, ids_ref[place : place + 1, :] == number)
    raised = jnp.where(named, jnp.exp(logits), 0.0)
    gates = raised / jnp.sum(raised, axis=0, keepdims=True)
    high = gates.astype(jnp.bfloat16).astype(jnp.float32)
    low = gates - high
    spare = jnp.zeros((padded - width - 2 * experts, rows), jnp.float32)
    extra = jnp.concatenate([high, low, spare], axis=0).T.astype(jnp.bfloat16)

    def spot(core, column, place):
        return pl.multiple_of(((core * 2 + column) * line + place) * R, R)

    mine = pl.ds(spot(c, y, z), R)
    for k in range(chunks):
        gath[k, mine, 0:width] = normed[k * R : (k + 1) * R]
        gath[k, mine, width:padded] = extra[k * R : (k + 1) * R]

    pl.semaphore_wait(barrier, line + 1)

    span = 2 * line - 1
    started = []
    gathered = [[] for _ in range(chunks)]
    scattered = [[] for _ in range(chunks)]

    def drain(pending):
        while pending:
            cond, copy = pending.pop(0)
            guarded(cond(), lambda: copy().wait_send())

    def label(side, offset):
        return side * span + offset + line - 1

    columns = [pl.ds(gather_cut, padded - gather_cut), pl.ds(0, gather_cut)]

    def slab(k, lot, side, offset, core=None):
        column = y if side == 0 else 1 - y
        core = c if core is None else core
        return gath.at[k, pl.ds(spot(core, column, z + offset), R), columns[lot]]

    def ag_copy(k, lot, side, offset, way):
        if way == RIGHT:
            landing = label(side, offset - 1)
        elif way == LEFT:
            landing = label(side, offset + 1)
        else:
            landing = label(1 - side, offset)
        where = slab(k, lot, side, offset)
        return pltpu.make_async_remote_copy(
            src_ref=where, dst_ref=where,
            send_sem=ag_send.at[k, lot, label(side, offset), way],
            recv_sem=ag_recv.at[k, lot, landing],
            device_id={"dev": dest[way]}, device_id_type=MESH,
        )

    def ag_ways(lot, side, offset):
        ways = []
        if lot == 0:
            if side == 0:
                if offset <= 0 and offset > 1 - line:
                    ways.append(RIGHT)
                if offset >= 0 and offset < line - 1:
                    ways.append(LEFT)
                ways.append(YMATE)
        else:
            if side == 0 and offset == 0:
                ways.append(YMATE)
            if offset <= 0 and offset > 1 - line:
                ways.append(RIGHT)
            if offset >= 0 and offset < line - 1:
                ways.append(LEFT)
        return ways

    def ag_step(k, lot, side, offset):
        def body():
            if side or offset:
                arrived = slab(k, lot, side, offset)
                pltpu.make_async_remote_copy(
                    src_ref=arrived, dst_ref=arrived,
                    send_sem=ag_send.at[k, lot, label(side, offset), YMATE],
                    recv_sem=ag_recv.at[k, lot, label(side, offset)],
                    device_id={"dev": dest[MATE]}, device_id_type=MESH,
                ).wait_recv()
            for way in ag_ways(lot, side, offset):
                guarded(allowed[way], ag_copy(k, lot, side, offset, way).start)

        guarded(exists(offset), body)
        for way in ag_ways(lot, side, offset):
            gathered[k].append(
                (
                    lambda way=way: both(exists(offset), allowed[way]),
                    lambda way=way: ag_copy(k, lot, side, offset, way),
                )
            )

    def ag_stage(k, stage):
        for lot in range(2):
            if stage == 0:
                ag_step(k, lot, 0, 0)
                continue
            if stage < line:
                ag_step(k, lot, 0, -stage)
                ag_step(k, lot, 0, stage)
            if stage == 1:
                ag_step(k, lot, 1, 0)
            else:
                ag_step(k, lot, 1, 1 - stage)
                ag_step(k, lot, 1, stage - 1)
        if stage >= line - 1:
            ag_pass(k, stage - line + 1).start()
            gathered[k].append((lambda: None, lambda: ag_pass(k, stage - line + 1)))

    def ag_pass(k, side, core=None):
        column = y if side == 0 else 1 - y
        core = c if core is None else core
        where = gath.at[k, pl.ds(spot(core, column, 0), line * R), :]
        return pltpu.make_async_remote_copy(
            src_ref=where, dst_ref=where,
            send_sem=pass_send.at[k, side], recv_sem=pass_recv.at[k, side],
            device_id={"dev": dest[MATE]}, device_id_type=MESH,
        )

    def mate_wait(k):
        for side in range(2):
            ag_pass(k, side, 1 - c).wait_recv()

    core_rows = total // 2
    strip = math.gcd(hidden, 256)

    wide = math.gcd(width, 512)

    def rise(k, start):
        if start == 0:
            if k == 0:
                for copy in copies:
                    copy.wait()
            mate_wait(k)
        x = gath[k, :, 0:width]
        if True:
            gate = jnp.dot(x, gu[:, start : start + strip], preferred_element_type=jnp.float32)
            up = jnp.dot(
                x, gu[:, hidden + start : hidden + start + strip],
                preferred_element_type=jnp.float32,
            )
            act[k, :, start : start + strip] = (gate / (1.0 + jnp.exp(-gate)) * up).astype(act.dtype)

    def fall(k, start):
        tail = gath[k, :, width:padded].astype(jnp.float32)
        lanes = lax.broadcasted_iota(jnp.int32, tail.shape, 1)
        chosen = jnp.logical_or(lanes == me, lanes == me + experts)
        weight = jnp.sum(jnp.where(chosen, tail, 0.0), axis=1, keepdims=True)
        if True:
            produced = jnp.dot(
                act[k], dn[:, start : start + wide], preferred_element_type=jnp.float32
            )
            made[k, :, start : start + wide] = (weight * produced).astype(made.dtype)
        if start + wide == width:
            mate_copy(k).start()
            scattered[k].append((lambda: None, lambda: mate_copy(k)))

    def mate_copy(k):
        theirs = pl.ds(pl.multiple_of((1 - c) * core_rows, core_rows), core_rows)
        return pltpu.make_async_remote_copy(
            src_ref=made.at[k, theirs, :], dst_ref=mrecv.at[k],
            send_sem=m_send.at[k], recv_sem=m_recv.at[k],
            device_id={"dev": dest[MATE]}, device_id_type=MESH,
        )

    late = pl.ds(0, scatter_cut)
    soon = pl.ds(scatter_cut, width - scatter_cut)

    def y_copy(k, lot):
        if lot == 0:
            source, target = part.at[k, 1 - y, :, :, soon], yrecv.at[k]
        else:
            source, target = ready.at[k], ylate.at[k]
        return pltpu.make_async_remote_copy(
            src_ref=source, dst_ref=target,
            send_sem=y_send.at[k, lot], recv_sem=y_recv.at[k, lot],
            device_id={"dev": dest[YMATE]}, device_id_type=MESH,
        )

    def y_start(k, lot):
        y_copy(k, lot).start()
        pending = scattered[k] if lot == 0 else started
        pending.append((lambda: None, lambda: y_copy(k, lot)))

    def z_copy(k, lot, offset):
        target = jnp.clip(z + offset, 0, line - 1)
        slot = line - 1 - offset
        if lot == 0:
            source, landing = half.at[k, target], zrecv.at[k, slot]
        else:
            source, landing = part.at[k, :, target, :, late], zearly.at[k, slot]
        return pltpu.make_async_remote_copy(
            src_ref=source, dst_ref=landing,
            send_sem=z_send.at[k, lot, line - 1 + offset], recv_sem=z_recv.at[k, lot, slot],
            device_id={"dev": me + 4 * (target - z)}, device_id_type=MESH,
        )

    def z_arrive(k, lot, offset):
        slot = line - 1 + offset
        where = (zrecv if lot == 0 else zearly).at[k, slot]
        pltpu.make_async_remote_copy(
            src_ref=where, dst_ref=where,
            send_sem=z_send.at[k, lot, slot], recv_sem=z_recv.at[k, lot, slot],
            device_id={"dev": dest[MATE]}, device_id_type=MESH,
        ).wait_recv()

    def z_start(k, lot):
        for offset in offsets:
            pl.when(exists(offset))(lambda offset=offset: z_copy(k, lot, offset).start())
            pending = scattered[k] if lot == 1 else started
            pending.append(
                (lambda offset=offset: exists(offset), lambda offset=offset: z_copy(k, lot, offset))
            )

    def merge(k):
        drain(gathered[k])
        mate_copy(k).wait_recv()
        for column in range(2):
            for place in range(line):
                at = column * line + place
                ours = pl.ds(pl.multiple_of(c * core_rows + at * R, R), R)
                part[k, column, place] = (
                    made[k, ours, :].astype(jnp.float32)
                    + mrecv[k, at * R : (at + 1) * R, :].astype(jnp.float32)
                ).astype(part.dtype)
        y_start(k, 0)
        z_start(k, 1)

    def middle(k):
        y_copy(k, 0).wait_recv()
        for place in range(line):
            half[k, place] = (
                part[k, y, place, :, soon].astype(jnp.float32)
                + yrecv[k, place].astype(jnp.float32)
            ).astype(half.dtype)
        z_start(k, 0)
        where = pl.ds(k * R, R)
        cross[...] = part[k, 1 - y, z, :, late].astype(jnp.float32)
        held[where, late] = held[where, late] + part[k, y, z, :, late].astype(jnp.float32)
        for offset in reversed(offsets):

            def add(offset=offset):
                z_arrive(k, 1, offset)
                slot = line - 1 + offset
                cross[...] = cross[...] + zearly[k, slot, 1 - y].astype(jnp.float32)
                held[where, late] = held[where, late] + zearly[k, slot, y].astype(jnp.float32)

            pl.when(exists(offset))(add)
        ready[k] = cross[...].astype(ready.dtype)
        y_start(k, 1)

    def finish(k):
        drain(scattered[k])
        where = pl.ds(k * R, R)
        held[where, soon] = held[where, soon] + half[k, z].astype(jnp.float32)
        for offset in reversed(offsets):

            def add(offset=offset):
                z_arrive(k, 0, offset)
                held[where, soon] = held[where, soon] + zrecv[k, line - 1 + offset].astype(
                    jnp.float32
                )

            pl.when(exists(offset))(add)
        y_copy(k, 1).wait_recv()
        held[where, late] = held[where, late] + ylate[k].astype(jnp.float32)
        o_ref[where, :] = held[where, :].astype(o_ref.dtype)

    rs_stages = [merge, middle, finish]
    pieces = [functools.partial(rise, start=start) for start in range(0, hidden, strip)]
    pieces += [functools.partial(fall, start=start) for start in range(0, width, wide)]
    queues = []
    for k in range(chunks):
        steps = [functools.partial(ag_stage, k, stage) for stage in range(line + 1)]
        steps += [functools.partial(piece, k) for piece in pieces]
        steps += [functools.partial(step, k) for step in rs_stages]
        queues.append(steps)
    order = ORDER
    if [order.count(k) for k in range(chunks)] != [len(steps) for steps in queues]:
        order = plain_order([len(steps) for steps in queues], line + 1 + len(pieces) // 2)
    for k in order:
        queues[k].pop(0)()
    drain(started)


def moe(attended, residual, gain, router, ids, gate_up, down, collective_id):
    devices = lax.axis_size("dev")
    rows, width = residual.shape
    hidden = down.shape[1]
    experts = router.shape[0]
    line = devices // 4
    padded = width + -(-2 * experts // 128) * 128
    R = rows // CHUNKS
    kind = residual.dtype
    span = 2 * line - 1
    vmem = pl.BlockSpec(memory_space=pltpu.VMEM)
    hbm = pl.BlockSpec(memory_space=pl.ANY)
    dma = pltpu.SemaphoreType.DMA
    total = devices * R
    gather_cut = width * GATHER_SHARE // 16 // 128 * 128
    scatter_cut = width * SCATTER_SHARE // 16 // 128 * 128
    soon = width - scatter_cut
    return pl.pallas_call(
        functools.partial(moe_kernel, line, gather_cut, scatter_cut),
        out_shape=jax.ShapeDtypeStruct((rows, width), kind),
        in_specs=[vmem] * 5 + [hbm] * 2,
        out_specs=vmem,
        scratch_shapes=[
            pltpu.VMEM((CHUNKS, total, padded), kind),
            pltpu.VMEM(gate_up.shape[1:], kind),
            pltpu.VMEM(down.shape[1:], kind),
            pltpu.VMEM((CHUNKS, total, hidden), kind),
            pltpu.VMEM((CHUNKS, total, width), kind),
            pltpu.VMEM((CHUNKS, total // 2, width), kind),
            pltpu.VMEM((CHUNKS, 2, line, R, width), kind),
            pltpu.VMEM((CHUNKS, line, R, soon), kind),
            pltpu.VMEM((CHUNKS, line, R, soon), kind),
            pltpu.VMEM((CHUNKS, span, R, soon), kind),
            pltpu.VMEM((rows, width), jnp.float32),
            pltpu.VMEM((CHUNKS, R, scatter_cut), kind),
            pltpu.VMEM((CHUNKS, R, scatter_cut), kind),
            pltpu.VMEM((CHUNKS, span, 2, R, scatter_cut), kind),
            pltpu.VMEM((R, scatter_cut), jnp.float32),
            dma((2,)),
            dma((CHUNKS, 2, 2 * span, 3)),
            dma((CHUNKS, 2, 2 * span)),
            dma((CHUNKS, 2)),
            dma((CHUNKS, 2)),
            dma((CHUNKS,)),
            dma((CHUNKS,)),
            dma((CHUNKS, 2)),
            dma((CHUNKS, 2)),
            dma((CHUNKS, 2, span)),
            dma((CHUNKS, 2, span)),
        ],
        compiler_params=pltpu.CompilerParams(collective_id=collective_id, has_side_effects=True),
    )(attended, residual, gain, router, ids, gate_up, down)


def swapped(order, one, two):
    order = list(order)
    order[one], order[two] = order[two], order[one]
    return order


def per_device(
    queries,
    key_values,
    lengths,
    out_proj,
    residual,
    norm_gain,
    router,
    expert_ids,
    expert_gate_up,
    expert_down,
):
    devices = lax.axis_size("dev")
    my_index = lax.axis_index("dev")
    width = residual.shape[-1]
    requests_n = devices // GROUP
    low_bits = bit_count(requests_n)
    near = list(range(bit_count(GROUP)))
    attended = attention(
        lengths, queries[0], key_values[:, 0], out_proj, low_bits, [near, swapped(near, 0, 1)], 1
    )
    if moe_fits(devices, TOK_DEV, width, FF):
        return moe(
            attended, residual[0], norm_gain, router.T, expert_ids[0].T,
            expert_gate_up, expert_down, 2,
        )[None]
    stream = (residual[0].astype(jnp.float32) + attended).astype(jnp.bfloat16)
    values = stream.astype(jnp.float32)
    normed = (
        values
        * lax.rsqrt(jnp.mean(values * values, axis=-1, keepdims=True) + EPSILON)
        * norm_gain.astype(jnp.float32)
    ).astype(jnp.bfloat16)
    logits = jnp.dot(normed, router, preferred_element_type=jnp.float32)
    experts_n = router.shape[1]
    token_ids = expert_ids[0]
    named = jnp.any(token_ids[..., None] == jnp.arange(experts_n, dtype=jnp.int32), axis=1)
    raised_gate = jnp.where(named, jnp.exp(logits), 0.0)
    gates = raised_gate / jnp.sum(raised_gate, axis=-1, keepdims=True)
    lanes = -(-TOK_DEV // 128) * 128
    gates = jnp.pad(gates.T, ((0, 0), (0, lanes - TOK_DEV)))
    every = list(range(bit_count(devices)))
    far = every[::-1]
    count = len(far)
    rows_all, gates_all = all_gather(normed, gates, [far, swapped(far, count - 3, count - 2)], 2)
    my_gates = lax.dynamic_index_in_dim(gates_all, my_index, 1, keepdims=False)[:, :TOK_DEV]
    flat_rows = rows_all.reshape(devices * TOK_DEV, width)
    projected = jnp.dot(flat_rows, expert_gate_up[0], preferred_element_type=jnp.float32)
    activation = (jax.nn.silu(projected[:, :FF]) * projected[:, FF:]).astype(jnp.bfloat16)
    produced = jnp.dot(activation, expert_down[0], preferred_element_type=jnp.float32)
    weighted = (my_gates.reshape(-1, 1) * produced).astype(jnp.bfloat16)
    weighted = weighted.reshape(devices, TOK_DEV, width)
    combined = reduce_scatter(weighted, 0, [every, swapped(every, 1, 2)], 3)
    return (values + combined).astype(jnp.bfloat16)[None]


def solution(mesh):
    return jax.shard_map(
        per_device,
        mesh=mesh,
        in_specs=(
            P(("groups", "dev"), None, None),
            P(None, ("groups", "dev"), None, None),
            P("groups"),
            P("dev", None),
            P(("groups", "dev"), None, None),
            P(),
            P(),
            P(("groups", "dev"), None, None),
            P("dev", None, None),
            P("dev", None, None),
        ),
        out_specs=P(("groups", "dev"), None, None),
        check_vma=False,
    )
```

```python
import functools
import math

import jax
import jax.numpy as jnp
from jax import lax
from jax.experimental import pallas as pl
from jax.experimental.pallas import tpu as pltpu
from jax.sharding import PartitionSpec as P

HEAD_DIM = 128
FF = 768
TOK_DEV = 64
GROUP = 8
EPSILON = 1e-06
MESH = pl.DeviceIdType.MESH
CHUNKS = 4
ATTENTION_GROUPS = 8
GATHER_SHARE = 7
SCATTER_SHARE = 3
ORDER = (
    0, 1, 0, 2, 0, 1, 0, 2, 0, 3, 0, 1, 0, 0, 0, 0, 2, 0, 0, 1, 3, 2, 0, 1,
    3, 2, 1, 1, 1, 1, 1, 1, 1, 2, 2, 2, 2, 0, 2, 3, 2, 2, 1, 3, 2, 3, 3, 3,
    3, 3, 3, 3, 1, 0, 3, 2, 3, 1, 2, 3,
)


def bit_count(number):
    return number.bit_length() - 1


def flipped(index, bits):
    for bit in bits:
        index = index + (1 - 2 * ((index // (1 << bit)) % 2)) * (1 << bit)
    return index


def subset(bits, number):
    return [bit for place, bit in enumerate(bits) if number >> place & 1]


def greet(me, bits):
    barrier = pltpu.get_barrier_semaphore()
    for bit in bits:
        pl.semaphore_signal(
            barrier, inc=1, device_id={"dev": flipped(me, [bit])}, device_id_type=MESH
        )
    pl.semaphore_wait(barrier, len(bits))


def scatter_steps(me, unit, part_no, order, cols, x_ref, recv, stage, send_sem, recv_sem, block_of):
    k = len(order)
    total = (1 << k) - 1
    first = [total - ((1 << (k - s)) - 1) for s in range(k)]

    def arrived(step, number):
        return pltpu.make_async_remote_copy(
            src_ref=recv.at[first[step] + number, :, cols],
            dst_ref=recv.at[first[step] + number, :, cols],
            send_sem=send_sem.at[part_no, first[step] + number],
            recv_sem=recv_sem.at[part_no, first[step] + number],
            device_id={"dev": flipped(me, [unit + order[step]])},
            device_id_type=MESH,
        )

    copies = []

    def send(step, only=None):
        for number in reversed(range(1 << (k - 1 - step))) if only is None else [only]:
            slot = first[step] + number
            flips = [order[step]] + subset(order[step + 1 :], number)
            block = block_of(flips)
            if step == 0:
                source = x_ref.at[block, :, cols]
            else:
                value = x_ref[block, :, cols].astype(jnp.float32)
                for earlier in range(step):
                    place = (1 << (step - earlier - 1)) + (number << (step - earlier))
                    arrived(earlier, place).wait_recv()
                    value = value + recv[first[earlier] + place, :, cols].astype(jnp.float32)
                spot = slot - first[1]
                stage[spot, :, cols] = value.astype(stage.dtype)
                source = stage.at[spot, :, cols]
            copy = pltpu.make_async_remote_copy(
                src_ref=source,
                dst_ref=recv.at[slot, :, cols],
                send_sem=send_sem.at[part_no, slot],
                recv_sem=recv_sem.at[part_no, slot],
                device_id={"dev": flipped(me, [unit + order[step]])},
                device_id_type=MESH,
            )
            copy.start()
            copies.append(copy)

    def finish(o_ref):
        value = x_ref[block_of([]), :, cols].astype(jnp.float32)
        for earlier in range(k):
            arrived(earlier, 0).wait_recv()
            value = value + recv[first[earlier], :, cols].astype(jnp.float32)
        o_ref[:, cols] = value
        for copy in copies:
            copy.wait_send()

    return send, finish


def scatter_kernel(unit, parts, bits, x_ref, o_ref, recv, stage, send_sem, recv_sem):
    me = lax.axis_index("dev")
    greet(me, [unit + bit for bit in bits])
    rank = me // (1 << unit)
    runs = [
        scatter_steps(
            me, unit, number, order, cols, x_ref, recv, stage, send_sem, recv_sem,
            lambda flips: flipped(rank, flips),
        )
        for number, (order, cols) in enumerate(parts)
    ]
    for step in range(len(bits)):
        for send, _ in runs:
            send(step)
    for _, finish in runs:
        finish(o_ref)


def attend_block(block, length, q_ref, halves, rows, values_ready=None):
    heads = q_ref.shape[1] // HEAD_DIM
    picked = pl.ds(pl.multiple_of(block * rows, rows), rows)
    query = jnp.concatenate(
        [q_ref[picked, head * HEAD_DIM : (head + 1) * HEAD_DIM] for head in range(heads)], axis=0
    )
    scale = 1.0 / math.sqrt(HEAD_DIM)
    contract = (((1,), (1,)), ((), ()))
    old = lax.dot_general(query, halves[0, 0], contract, preferred_element_type=jnp.float32) * scale
    new = lax.dot_general(query, halves[1, 0], contract, preferred_element_type=jnp.float32) * scale
    column = lax.broadcasted_iota(jnp.int32, (1, old.shape[1]), 1)
    old = jnp.where(column < length, old, -1e30)
    column = lax.broadcasted_iota(jnp.int32, (rows, new.shape[1]), 1)
    token = lax.broadcasted_iota(jnp.int32, (rows, new.shape[1]), 0) + block * rows
    bias = jnp.where(column <= token, 0.0, -1e30)
    new = new + jnp.concatenate([bias] * heads, axis=0)
    top = jnp.maximum(jnp.max(old, axis=1, keepdims=True), jnp.max(new, axis=1, keepdims=True))
    old = jnp.exp(old - top)
    new = jnp.exp(new - top)
    total = jnp.sum(old, axis=1, keepdims=True) + jnp.sum(new, axis=1, keepdims=True)
    if values_ready is not None:
        values_ready()
    mixed = jnp.dot(old.astype(jnp.bfloat16), halves[0, 1], preferred_element_type=jnp.float32)
    mixed += jnp.dot(new.astype(jnp.bfloat16), halves[1, 1], preferred_element_type=jnp.float32)
    mixed = (mixed / total).astype(jnp.bfloat16)
    return jnp.concatenate(
        [mixed[head * rows : (head + 1) * rows] for head in range(heads)], axis=1
    )


def attention_kernel(
    unit, parts, bits,
    lengths_ref, q_ref, kv_ref, proj_ref, o_ref,
    halves, proj, heads, x, recv, stage,
    send_sem, recv_sem, kv_sem, proj_send, proj_recv, own_sem,
):
    me = lax.axis_index("dev")
    low = list(range(unit))
    mates = [flipped(me, subset(low, number)) for number in range(1, 1 << unit)]
    ranks = [flipped(me, [unit + bit]) for bit in bits]
    barrier = pltpu.get_barrier_semaphore()
    for other in mates + ranks:
        pl.semaphore_signal(barrier, inc=1, device_id={"dev": other}, device_id_type=MESH)
    request = me % (1 << unit)
    rank = me // (1 << unit)
    parity = rank % 2
    depth = proj_ref.shape[0]
    own_rows = pl.ds(pl.multiple_of(request * depth, depth), depth)
    own_half = pltpu.make_async_copy(kv_ref, halves.at[parity], own_sem.at[0])
    own_proj = pltpu.make_async_copy(proj_ref, proj.at[own_rows], own_sem.at[1])
    own_half.start()
    own_proj.start()
    pl.semaphore_wait(barrier, len(mates) + len(ranks))
    kv_copies = [
        pltpu.make_async_remote_copy(
            src_ref=kv_ref.at[place],
            dst_ref=halves.at[parity, place],
            send_sem=kv_sem.at[place],
            recv_sem=kv_sem.at[2 + place],
            device_id={"dev": ranks[0]},
            device_id_type=MESH,
        )
        for place in range(2)
    ]
    for copy in kv_copies:
        copy.start()
    proj_copies = []
    for place, other in enumerate(mates):
        copy = pltpu.make_async_remote_copy(
            src_ref=proj_ref,
            dst_ref=proj.at[own_rows],
            send_sem=proj_send.at[place],
            recv_sem=proj_recv.at[place],
            device_id={"dev": other},
            device_id_type=MESH,
        )
        copy.start()
        proj_copies.append(copy)
    own_half.wait()
    kv_copies[0].wait()

    blocks, rows, width = x.shape
    far = 1 << (len(bits) - 1)
    masks = sorted(range(blocks), key=lambda m: (-bin(m).count("1"), -(m & far), m))
    place_of = {mask: place for place, mask in enumerate(masks)}
    length = lengths_ref[request]
    runs = [
        scatter_steps(
            me, unit, number, order, cols, x, recv, stage, send_sem, recv_sem,
            lambda flips: place_of[sum(1 << bit for bit in flips)],
        )
        for number, (order, cols) in enumerate(parts)
    ]
    groups = min(ATTENTION_GROUPS, blocks)
    half = blocks // groups
    strip = math.gcd(width, 512)
    for group in range(groups):
        for spot in range(half):
            mask = masks[group * half + spot]
            block = flipped(rank, subset(bits, mask))
            heads[spot * rows : (spot + 1) * rows, :] = attend_block(
                block, length, q_ref, halves, rows,
                kv_copies[1].wait if group == 0 and spot == 0 else None,
            )
        if group == 0:
            own_proj.wait()
            for copy in proj_copies:
                copy.wait()
        for start in range(0, width, strip):
            product = jnp.dot(
                heads[...], proj[:, start : start + strip], preferred_element_type=jnp.float32
            ).astype(x.dtype)
            for spot in range(half):
                x[group * half + spot, :, start : start + strip] = product[
                    spot * rows : (spot + 1) * rows
                ]
        for spot in range(half):
            mask = masks[group * half + spot]
            for (send, _), (order, _) in zip(runs, parts):
                if mask >> order[0] & 1:
                    number = sum((mask >> bit & 1) << at for at, bit in enumerate(order[1:]))
                    send(0, number)
    for step in range(1, len(bits)):
        for send, _ in runs:
            send(step)
    for _, finish in runs:
        finish(o_ref)


def attention(lengths, queries, key_values, out_proj, unit, orders, collective_id):
    width = out_proj.shape[1]
    tokens, columns = queries.shape
    bits = sorted(orders[0])
    blocks = 1 << len(bits)
    rows = tokens // blocks
    cut = width * 13 // 16 // 128 * 128
    parts = [(orders[0], pl.ds(0, cut)), (orders[1], pl.ds(cut, width - cut))]
    mates = max((1 << unit) - 1, 1)
    kind = queries.dtype
    whole = pl.BlockSpec(memory_space=pltpu.VMEM)
    return pl.pallas_call(
        functools.partial(attention_kernel, unit, parts, bits),
        out_shape=jax.ShapeDtypeStruct((rows, width), jnp.float32),
        in_specs=[pl.BlockSpec(memory_space=pltpu.SMEM), whole, whole, whole],
        out_specs=whole,
        scratch_shapes=[
            pltpu.VMEM((2,) + key_values.shape, kind),
            pltpu.VMEM((out_proj.shape[0] << unit, width), kind),
            pltpu.VMEM((tokens // min(ATTENTION_GROUPS, blocks), columns), kind),
            pltpu.VMEM((blocks, rows, width), kind),
            pltpu.VMEM((blocks - 1, rows, width), kind),
            pltpu.VMEM((max(blocks // 2 - 1, 1), rows, width), kind),
            pltpu.SemaphoreType.DMA((2, blocks - 1)),
            pltpu.SemaphoreType.DMA((2, blocks - 1)),
            pltpu.SemaphoreType.DMA((4,)),
            pltpu.SemaphoreType.DMA((mates,)),
            pltpu.SemaphoreType.DMA((mates,)),
            pltpu.SemaphoreType.DMA((2,)),
        ],
        compiler_params=pltpu.CompilerParams(collective_id=collective_id, has_side_effects=True),
    )(lengths, queries, key_values, out_proj)


def reduce_scatter(x, unit, orders, collective_id):
    blocks, rows, width = x.shape
    bits = sorted(orders[0])
    cut = width * 3 // 4 // 128 * 128
    parts = [(orders[0], pl.ds(0, cut)), (orders[1], pl.ds(cut, width - cut))]
    return pl.pallas_call(
        functools.partial(scatter_kernel, unit, parts, bits),
        out_shape=jax.ShapeDtypeStruct((rows, width), jnp.float32),
        in_specs=[pl.BlockSpec(memory_space=pltpu.VMEM)],
        out_specs=pl.BlockSpec(memory_space=pltpu.VMEM),
        scratch_shapes=[
            pltpu.VMEM((blocks - 1, rows, width), x.dtype),
            pltpu.VMEM((max(blocks // 2 - 1, 1), rows, width), x.dtype),
            pltpu.SemaphoreType.DMA((2, blocks - 1)),
            pltpu.SemaphoreType.DMA((2, blocks - 1)),
        ],
        compiler_params=pltpu.CompilerParams(collective_id=collective_id, has_side_effects=True),
    )(x)


def gather_kernel(parts, bits, x_ref, g_ref, ox_ref, og_ref, send_sem, recv_sem, own_sem):
    me = lax.axis_index("dev")
    greet(me, bits)
    k = len(bits)
    pairs = [(x_ref, ox_ref), (g_ref, og_ref)]
    local = []
    for number, (source, target) in enumerate(pairs):
        copy = pltpu.make_async_copy(source, target.at[me], own_sem.at[number])
        copy.start()
        local.append(copy)
    sent = []

    def forward(part_no, held, step):
        which, order, cols = parts[part_no]
        source, target = pairs[which]
        block = flipped(me, subset(order, held))
        slot = (1 << step) - 1 + held
        copy = pltpu.make_async_remote_copy(
            src_ref=source.at[:, cols] if held == 0 else target.at[block, :, cols],
            dst_ref=target.at[block, :, cols],
            send_sem=send_sem.at[part_no, slot],
            recv_sem=recv_sem.at[part_no, slot],
            device_id={"dev": flipped(me, [order[step]])},
            device_id_type=MESH,
        )
        copy.start()
        sent.append(copy)

    def arrive(part_no, held, step):
        which, order, cols = parts[part_no]
        target = pairs[which][1]
        block = flipped(me, subset(order, held) + [order[step]])
        slot = (1 << step) - 1 + held
        pltpu.make_async_remote_copy(
            src_ref=target.at[block, :, cols],
            dst_ref=target.at[block, :, cols],
            send_sem=send_sem.at[part_no, slot],
            recv_sem=recv_sem.at[part_no, slot],
            device_id={"dev": flipped(me, [order[step]])},
            device_id_type=MESH,
        ).wait_recv()

    for step in range(k):
        for part_no in range(len(parts)):
            forward(part_no, 0, step)
    for step in range(k):
        for held in range(1 << step):
            for part_no in range(len(parts)):
                arrive(part_no, held, step)
                for later in range(step + 1, k):
                    forward(part_no, held + (1 << step), later)
    for copy in local:
        copy.wait()
    for copy in sent:
        copy.wait_send()


def all_gather(x, gates, orders, collective_id):
    rows, width = x.shape
    bits = sorted(orders[0])
    count = 1 << len(bits)
    cut = width * 3 // 4 // 128 * 128
    parts = [
        (1, orders[0], pl.ds(0, gates.shape[1])),
        (0, orders[0], pl.ds(0, cut)),
        (0, orders[1], pl.ds(cut, width - cut)),
    ]
    return pl.pallas_call(
        functools.partial(gather_kernel, parts, bits),
        out_shape=[
            jax.ShapeDtypeStruct((count, rows, width), x.dtype),
            jax.ShapeDtypeStruct((count,) + gates.shape, gates.dtype),
        ],
        in_specs=[pl.BlockSpec(memory_space=pltpu.VMEM)] * 2,
        out_specs=[pl.BlockSpec(memory_space=pltpu.VMEM)] * 2,
        scratch_shapes=[
            pltpu.SemaphoreType.DMA((3, count - 1)),
            pltpu.SemaphoreType.DMA((3, count - 1)),
            pltpu.SemaphoreType.DMA((2,)),
        ],
        compiler_params=pltpu.CompilerParams(collective_id=collective_id, has_side_effects=True),
    )(x, gates)


def plain_order(counts, lag):
    entries = [(step + lag * k, k) for k, count in enumerate(counts) for step in range(count)]
    return [k for _, k in sorted(entries)]


def moe_fits(devices, rows, width, hidden):
    if devices < 8 or rows % (16 * CHUNKS):
        return False
    weights = 3 * width * hidden
    tokens = devices * rows * width
    return 2 * (weights + 4 * tokens) < 48 * 2**20


def moe_kernel(
    line, gather_cut, scatter_cut,
    att_ref, res_ref, gain_ref, router_ref, ids_ref, gu_hbm, dn_hbm, o_ref,
    gath, gu, dn, act, made, mrecv, part, yrecv, half, zrecv, held, ready, ylate, zearly, cross,
    w_sem, ag_send, ag_recv, pass_send, pass_recv, m_send, m_recv, y_send, y_recv, z_send, z_recv,
):
    me = lax.axis_index("dev")
    z, y, c = me // 4, (me // 2) % 2, me % 2
    chunks, total, padded = gath.shape
    rows, width = o_ref.shape
    R = rows // chunks
    hidden = dn.shape[0]
    experts = router_ref.shape[0]
    dest = [me + 4, me - 4, me + 2 - 4 * y, me + 1 - 2 * c]
    allowed = [z + 1 < line, z > 0, None, None]
    RIGHT, LEFT, YMATE, MATE = range(4)

    def guarded(cond, body):
        if cond is None:
            body()
        else:
            pl.when(cond)(body)

    def both(*conds):
        conds = [cond for cond in conds if cond is not None]
        if not conds:
            return None
        return functools.reduce(jnp.logical_and, conds)

    copies = [
        pltpu.make_async_copy(gu_hbm.at[0], gu, w_sem.at[0]),
        pltpu.make_async_copy(dn_hbm.at[0], dn, w_sem.at[1]),
    ]
    for copy in copies:
        copy.start()
    barrier = pltpu.get_barrier_semaphore()
    offsets = [sign * step for step in range(line - 1, 0, -1) for sign in (1, -1)]

    def exists(offset):
        if offset == 0:
            return None
        return z + offset >= 0 if offset < 0 else z + offset < line

    def greet_one(other):
        pl.semaphore_signal(barrier, inc=1, device_id={"dev": other}, device_id_type=MESH)

    greet_one(dest[YMATE])
    greet_one(dest[MATE])
    for offset in offsets:
        pl.when(exists(offset))(lambda offset=offset: greet_one(me + 4 * offset))

    stream = (res_ref[...].astype(jnp.float32) + att_ref[...]).astype(jnp.bfloat16)
    values = stream.astype(jnp.float32)
    held[...] = values
    scale = lax.rsqrt(jnp.mean(values * values, axis=-1, keepdims=True) + EPSILON)
    normed = (values * scale * gain_ref[...].astype(jnp.float32).reshape(1, width)).astype(jnp.bfloat16)
    logits = lax.dot_general(
        router_ref[...], normed, (((1,), (1,)), ((), ())), preferred_element_type=jnp.float32
    )
    number = lax.broadcasted_iota(jnp.int32, (experts, rows), 0)
    named = ids_ref[0:1, :] == number
    for place in range(1, ids_ref.shape[0]):
        named = jnp.logical_or(named, ids_ref[place : place + 1, :] == number)
    raised = jnp.where(named, jnp.exp(logits), 0.0)
    gates = raised / jnp.sum(raised, axis=0, keepdims=True)
    high = gates.astype(jnp.bfloat16).astype(jnp.float32)
    low = gates - high
    spare = jnp.zeros((padded - width - 2 * experts, rows), jnp.float32)
    extra = jnp.concatenate([high, low, spare], axis=0).T.astype(jnp.bfloat16)

    def spot(core, column, place):
        return pl.multiple_of(((core * 2 + column) * line + place) * R, R)

    mine = pl.ds(spot(c, y, z), R)
    for k in range(chunks):
        gath[k, mine, 0:width] = normed[k * R : (k + 1) * R]
        gath[k, mine, width:padded] = extra[k * R : (k + 1) * R]

    pl.semaphore_wait(barrier, line + 1)

    span = 2 * line - 1
    started = []
    gathered = [[] for _ in range(chunks)]
    scattered = [[] for _ in range(chunks)]

    def drain(pending):
        while pending:
            cond, copy = pending.pop(0)
            guarded(cond(), lambda: copy().wait_send())

    def label(side, offset):
        return side * span + offset + line - 1

    columns = [pl.ds(gather_cut, padded - gather_cut), pl.ds(0, gather_cut)]

    def slab(k, lot, side, offset, core=None):
        column = y if side == 0 else 1 - y
        core = c if core is None else core
        return gath.at[k, pl.ds(spot(core, column, z + offset), R), columns[lot]]

    def ag_copy(k, lot, side, offset, way):
        if way == RIGHT:
            landing = label(side, offset - 1)
        elif way == LEFT:
            landing = label(side, offset + 1)
        else:
            landing = label(1 - side, offset)
        where = slab(k, lot, side, offset)
        return pltpu.make_async_remote_copy(
            src_ref=where, dst_ref=where,
            send_sem=ag_send.at[k, lot, label(side, offset), way],
            recv_sem=ag_recv.at[k, lot, landing],
            device_id={"dev": dest[way]}, device_id_type=MESH,
        )

    def ag_ways(lot, side, offset):
        ways = []
        if lot == 0:
            if side == 0:
                if offset <= 0 and offset > 1 - line:
                    ways.append(RIGHT)
                if offset >= 0 and offset < line - 1:
                    ways.append(LEFT)
                ways.append(YMATE)
        else:
            if side == 0 and offset == 0:
                ways.append(YMATE)
            if offset <= 0 and offset > 1 - line:
                ways.append(RIGHT)
            if offset >= 0 and offset < line - 1:
                ways.append(LEFT)
        return ways

    def ag_step(k, lot, side, offset):
        def body():
            if side or offset:
                arrived = slab(k, lot, side, offset)
                pltpu.make_async_remote_copy(
                    src_ref=arrived, dst_ref=arrived,
                    send_sem=ag_send.at[k, lot, label(side, offset), YMATE],
                    recv_sem=ag_recv.at[k, lot, label(side, offset)],
                    device_id={"dev": dest[MATE]}, device_id_type=MESH,
                ).wait_recv()
            for way in ag_ways(lot, side, offset):
                guarded(allowed[way], ag_copy(k, lot, side, offset, way).start)

        guarded(exists(offset), body)
        for way in ag_ways(lot, side, offset):
            gathered[k].append(
                (
                    lambda way=way: both(exists(offset), allowed[way]),
                    lambda way=way: ag_copy(k, lot, side, offset, way),
                )
            )

    def ag_stage(k, stage):
        for lot in range(2):
            if stage == 0:
                ag_step(k, lot, 0, 0)
                continue
            if stage < line:
                ag_step(k, lot, 0, -stage)
                ag_step(k, lot, 0, stage)
            if stage == 1:
                ag_step(k, lot, 1, 0)
            else:
                ag_step(k, lot, 1, 1 - stage)
                ag_step(k, lot, 1, stage - 1)
        if stage >= line - 1:
            ag_pass(k, stage - line + 1).start()
            gathered[k].append((lambda: None, lambda: ag_pass(k, stage - line + 1)))

    def ag_pass(k, side, core=None):
        column = y if side == 0 else 1 - y
        core = c if core is None else core
        where = gath.at[k, pl.ds(spot(core, column, 0), line * R), :]
        return pltpu.make_async_remote_copy(
            src_ref=where, dst_ref=where,
            send_sem=pass_send.at[k, side], recv_sem=pass_recv.at[k, side],
            device_id={"dev": dest[MATE]}, device_id_type=MESH,
        )

    def mate_wait(k):
        for side in range(2):
            ag_pass(k, side, 1 - c).wait_recv()

    core_rows = total // 2
    strip = math.gcd(hidden, 256)

    wide = math.gcd(width, 512)

    def rise(k, start):
        if start == 0:
            if k == 0:
                for copy in copies:
                    copy.wait()
            mate_wait(k)
        x = gath[k, :, 0:width]
        if True:
            gate = jnp.dot(x, gu[:, start : start + strip], preferred_element_type=jnp.float32)
            up = jnp.dot(
                x, gu[:, hidden + start : hidden + start + strip],
                preferred_element_type=jnp.float32,
            )
            act[k, :, start : start + strip] = (gate / (1.0 + jnp.exp(-gate)) * up).astype(act.dtype)

    def fall(k, start):
        tail = gath[k, :, width:padded].astype(jnp.float32)
        lanes = lax.broadcasted_iota(jnp.int32, tail.shape, 1)
        chosen = jnp.logical_or(lanes == me, lanes == me + experts)
        weight = jnp.sum(jnp.where(chosen, tail, 0.0), axis=1, keepdims=True)
        if True:
            produced = jnp.dot(
                act[k], dn[:, start : start + wide], preferred_element_type=jnp.float32
            )
            made[k, :, start : start + wide] = (weight * produced).astype(made.dtype)
        if start + wide == width:
            mate_copy(k).start()
            scattered[k].append((lambda: None, lambda: mate_copy(k)))

    def mate_copy(k):
        theirs = pl.ds(pl.multiple_of((1 - c) * core_rows, core_rows), core_rows)
        return pltpu.make_async_remote_copy(
            src_ref=made.at[k, theirs, :], dst_ref=mrecv.at[k],
            send_sem=m_send.at[k], recv_sem=m_recv.at[k],
            device_id={"dev": dest[MATE]}, device_id_type=MESH,
        )

    late = pl.ds(0, scatter_cut)
    soon = pl.ds(scatter_cut, width - scatter_cut)

    def y_copy(k, lot):
        if lot == 0:
            source, target = part.at[k, 1 - y, :, :, soon], yrecv.at[k]
        else:
            source, target = ready.at[k], ylate.at[k]
        return pltpu.make_async_remote_copy(
            src_ref=source, dst_ref=target,
            send_sem=y_send.at[k, lot], recv_sem=y_recv.at[k, lot],
            device_id={"dev": dest[YMATE]}, device_id_type=MESH,
        )

    def y_start(k, lot):
        y_copy(k, lot).start()
        pending = scattered[k] if lot == 0 else started
        pending.append((lambda: None, lambda: y_copy(k, lot)))

    def z_copy(k, lot, offset):
        target = jnp.clip(z + offset, 0, line - 1)
        slot = line - 1 - offset
        if lot == 0:
            source, landing = half.at[k, target], zrecv.at[k, slot]
        else:
            source, landing = part.at[k, :, target, :, late], zearly.at[k, slot]
        return pltpu.make_async_remote_copy(
            src_ref=source, dst_ref=landing,
            send_sem=z_send.at[k, lot, line - 1 + offset], recv_sem=z_recv.at[k, lot, slot],
            device_id={"dev": me + 4 * (target - z)}, device_id_type=MESH,
        )

    def z_arrive(k, lot, offset):
        slot = line - 1 + offset
        where = (zrecv if lot == 0 else zearly).at[k, slot]
        pltpu.make_async_remote_copy(
            src_ref=where, dst_ref=where,
            send_sem=z_send.at[k, lot, slot], recv_sem=z_recv.at[k, lot, slot],
            device_id={"dev": dest[MATE]}, device_id_type=MESH,
        ).wait_recv()

    def z_start(k, lot):
        for offset in offsets:
            pl.when(exists(offset))(lambda offset=offset: z_copy(k, lot, offset).start())
            pending = scattered[k] if lot == 1 else started
            pending.append(
                (lambda offset=offset: exists(offset), lambda offset=offset: z_copy(k, lot, offset))
            )

    def merge(k):
        drain(gathered[k])
        mate_copy(k).wait_recv()
        for column in (1 - y, y):
            for place in range(line):
                at = column * line + place
                ours = pl.ds(pl.multiple_of(c * core_rows + at * R, R), R)
                theirs = pl.ds(pl.multiple_of(at * R, R), R)
                part[k, column, place] = (
                    made[k, ours, :].astype(jnp.float32) + mrecv[k, theirs, :].astype(jnp.float32)
                ).astype(part.dtype)
            if column is not y:
                y_start(k, 0)
        z_start(k, 1)

    def middle(k):
        y_copy(k, 0).wait_recv()
        for place in range(line):
            half[k, place] = (
                part[k, y, place, :, soon].astype(jnp.float32)
                + yrecv[k, place].astype(jnp.float32)
            ).astype(half.dtype)
        z_start(k, 0)
        where = pl.ds(k * R, R)
        cross[...] = part[k, 1 - y, z, :, late].astype(jnp.float32)
        held[where, late] = held[where, late] + part[k, y, z, :, late].astype(jnp.float32)
        for offset in reversed(offsets):

            def add(offset=offset):
                z_arrive(k, 1, offset)
                slot = line - 1 + offset
                cross[...] = cross[...] + zearly[k, slot, 1 - y].astype(jnp.float32)
                held[where, late] = held[where, late] + zearly[k, slot, y].astype(jnp.float32)

            pl.when(exists(offset))(add)
        ready[k] = cross[...].astype(ready.dtype)
        y_start(k, 1)

    def finish(k):
        drain(scattered[k])
        where = pl.ds(k * R, R)
        held[where, soon] = held[where, soon] + half[k, z].astype(jnp.float32)
        for offset in reversed(offsets):

            def add(offset=offset):
                z_arrive(k, 0, offset)
                held[where, soon] = held[where, soon] + zrecv[k, line - 1 + offset].astype(
                    jnp.float32
                )

            pl.when(exists(offset))(add)
        y_copy(k, 1).wait_recv()
        held[where, late] = held[where, late] + ylate[k].astype(jnp.float32)
        o_ref[where, :] = held[where, :].astype(o_ref.dtype)

    rs_stages = [merge, middle, finish]
    pieces = [functools.partial(rise, start=start) for start in range(0, hidden, strip)]
    pieces += [functools.partial(fall, start=start) for start in range(0, width, wide)]
    queues = []
    for k in range(chunks):
        steps = [functools.partial(ag_stage, k, stage) for stage in range(line + 1)]
        steps += [functools.partial(piece, k) for piece in pieces]
        steps += [functools.partial(step, k) for step in rs_stages]
        queues.append(steps)
    order = ORDER
    if [order.count(k) for k in range(chunks)] != [len(steps) for steps in queues]:
        order = plain_order([len(steps) for steps in queues], line + 1 + len(pieces) // 2)
    for k in order:
        queues[k].pop(0)()
    drain(started)


def moe(attended, residual, gain, router, ids, gate_up, down, collective_id):
    devices = lax.axis_size("dev")
    rows, width = residual.shape
    hidden = down.shape[1]
    experts = router.shape[0]
    line = devices // 4
    padded = width + -(-2 * experts // 128) * 128
    R = rows // CHUNKS
    kind = residual.dtype
    span = 2 * line - 1
    vmem = pl.BlockSpec(memory_space=pltpu.VMEM)
    hbm = pl.BlockSpec(memory_space=pl.ANY)
    dma = pltpu.SemaphoreType.DMA
    total = devices * R
    gather_cut = width * GATHER_SHARE // 16 // 128 * 128
    scatter_cut = width * SCATTER_SHARE // 16 // 128 * 128
    soon = width - scatter_cut
    return pl.pallas_call(
        functools.partial(moe_kernel, line, gather_cut, scatter_cut),
        out_shape=jax.ShapeDtypeStruct((rows, width), kind),
        in_specs=[vmem] * 5 + [hbm] * 2,
        out_specs=vmem,
        scratch_shapes=[
            pltpu.VMEM((CHUNKS, total, padded), kind),
            pltpu.VMEM(gate_up.shape[1:], kind),
            pltpu.VMEM(down.shape[1:], kind),
            pltpu.VMEM((CHUNKS, total, hidden), kind),
            pltpu.VMEM((CHUNKS, total, width), kind),
            pltpu.VMEM((CHUNKS, total // 2, width), kind),
            pltpu.VMEM((CHUNKS, 2, line, R, width), kind),
            pltpu.VMEM((CHUNKS, line, R, soon), kind),
            pltpu.VMEM((CHUNKS, line, R, soon), kind),
            pltpu.VMEM((CHUNKS, span, R, soon), kind),
            pltpu.VMEM((rows, width), jnp.float32),
            pltpu.VMEM((CHUNKS, R, scatter_cut), kind),
            pltpu.VMEM((CHUNKS, R, scatter_cut), kind),
            pltpu.VMEM((CHUNKS, span, 2, R, scatter_cut), kind),
            pltpu.VMEM((R, scatter_cut), jnp.float32),
            dma((2,)),
            dma((CHUNKS, 2, 2 * span, 3)),
            dma((CHUNKS, 2, 2 * span)),
            dma((CHUNKS, 2)),
            dma((CHUNKS, 2)),
            dma((CHUNKS,)),
            dma((CHUNKS,)),
            dma((CHUNKS, 2)),
            dma((CHUNKS, 2)),
            dma((CHUNKS, 2, span)),
            dma((CHUNKS, 2, span)),
        ],
        compiler_params=pltpu.CompilerParams(collective_id=collective_id, has_side_effects=True),
    )(attended, residual, gain, router, ids, gate_up, down)


def swapped(order, one, two):
    order = list(order)
    order[one], order[two] = order[two], order[one]
    return order


def per_device(
    queries,
    key_values,
    lengths,
    out_proj,
    residual,
    norm_gain,
    router,
    expert_ids,
    expert_gate_up,
    expert_down,
):
    devices = lax.axis_size("dev")
    my_index = lax.axis_index("dev")
    width = residual.shape[-1]
    requests_n = devices // GROUP
    low_bits = bit_count(requests_n)
    near = list(range(bit_count(GROUP)))
    attended = attention(
        lengths, queries[0], key_values[:, 0], out_proj, low_bits, [near, swapped(near, 0, 1)], 1
    )
    if moe_fits(devices, TOK_DEV, width, FF):
        return moe(
            attended, residual[0], norm_gain, router.T, expert_ids[0].T,
            expert_gate_up, expert_down, 2,
        )[None]
    stream = (residual[0].astype(jnp.float32) + attended).astype(jnp.bfloat16)
    values = stream.astype(jnp.float32)
    normed = (
        values
        * lax.rsqrt(jnp.mean(values * values, axis=-1, keepdims=True) + EPSILON)
        * norm_gain.astype(jnp.float32)
    ).astype(jnp.bfloat16)
    logits = jnp.dot(normed, router, preferred_element_type=jnp.float32)
    experts_n = router.shape[1]
    token_ids = expert_ids[0]
    named = jnp.any(token_ids[..., None] == jnp.arange(experts_n, dtype=jnp.int32), axis=1)
    raised_gate = jnp.where(named, jnp.exp(logits), 0.0)
    gates = raised_gate / jnp.sum(raised_gate, axis=-1, keepdims=True)
    lanes = -(-TOK_DEV // 128) * 128
    gates = jnp.pad(gates.T, ((0, 0), (0, lanes - TOK_DEV)))
    every = list(range(bit_count(devices)))
    far = every[::-1]
    count = len(far)
    rows_all, gates_all = all_gather(normed, gates, [far, swapped(far, count - 3, count - 2)], 2)
    my_gates = lax.dynamic_index_in_dim(gates_all, my_index, 1, keepdims=False)[:, :TOK_DEV]
    flat_rows = rows_all.reshape(devices * TOK_DEV, width)
    projected = jnp.dot(flat_rows, expert_gate_up[0], preferred_element_type=jnp.float32)
    activation = (jax.nn.silu(projected[:, :FF]) * projected[:, FF:]).astype(jnp.bfloat16)
    produced = jnp.dot(activation, expert_down[0], preferred_element_type=jnp.float32)
    weighted = (my_gates.reshape(-1, 1) * produced).astype(jnp.bfloat16)
    weighted = weighted.reshape(devices, TOK_DEV, width)
    combined = reduce_scatter(weighted, 0, [every, swapped(every, 1, 2)], 3)
    return (values + combined).astype(jnp.bfloat16)[None]


def solution(mesh):
    return jax.shard_map(
        per_device,
        mesh=mesh,
        in_specs=(
            P(("groups", "dev"), None, None),
            P(None, ("groups", "dev"), None, None),
            P("groups"),
            P("dev", None),
            P(("groups", "dev"), None, None),
            P(),
            P(),
            P(("groups", "dev"), None, None),
            P("dev", None, None),
            P("dev", None, None),
        ),
        out_specs=P(("groups", "dev"), None, None),
        check_vma=False,
    )
```
